8 devices in a mesh: vp: 8 (over z, y, x, core).
Axes of the slice: x: 2, y: 2, z: 1, core: 2. Of those that a mesh axis runs over, the one named last changes fastest.
Arguments:
- table_in: float32 [50304, 768], P('vp')
- table_out: float32 [50304, 768], P('vp')
- center_ids: int32 [65536], P('vp')
- context_ids: int32 [65536], P('vp')
- negative_ids: int32 [32768], P('vp')
Outputs:
- output 1: float32 [50304, 768], P('vp')
- output 2: float32 [50304, 768], P('vp')
All inputs are finite; a program needn't handle non-finite values.
Results may differ from the reference program's by a relative error of at most 0.001.
Values sent between devices are 32-bit elements.
A program may use at most 1 GiB of HBM per device.

```python
import jax
import jax.numpy as jnp
from jax import lax

VOCAB_SIZE = 50304
EMBED_DIM = 768
PAIRS_DEV = 8192
NEGATIVES = 4096
SHARDS = 8
ROWS_SHARD = VOCAB_SIZE // SHARDS
NEG_WEIGHT = 5.0
LEARN_RATE = 1.0
NEG_SCALE = NEG_WEIGHT / NEGATIVES


def draw_ids(base_key, num_ids):
    common_slots = 3 * num_ids // SHARDS
    common_rows = common_slots // 4
    span_rows = ROWS_SHARD - common_rows
    key_common, key_start, key_perm = jax.random.split(base_key, 3)
    slot_idx = jnp.arange(num_ids, dtype=jnp.int32)
    common_pick = jax.random.randint(key_common, (SHARDS, num_ids), 0, common_rows, dtype=jnp.int32)
    common_part = jnp.where(slot_idx < common_rows, slot_idx, common_pick)
    other_idx = jnp.maximum(slot_idx - common_slots, 0)
    shard_idx = other_idx % SHARDS
    rank_idx = other_idx // SHARDS
    starts = jax.random.randint(key_start, (SHARDS, SHARDS), 0, span_rows, dtype=jnp.int32)
    other_part = shard_idx * ROWS_SHARD + common_rows + (starts[:, shard_idx] + rank_idx) % span_rows
    id_table = jnp.where(slot_idx < common_slots, common_part, other_part)
    return jax.random.permutation(key_perm, id_table, axis=1, independent=True).reshape(-1)


def setup_inputs(seed: int = 0) -> dict:
    base_key = jax.random.key(seed)
    key_in, key_out, key_center, key_context, key_neg = jax.random.split(base_key, 5)
    row_scale = EMBED_DIM ** -0.25
    table_in = jax.random.normal(key_in, (VOCAB_SIZE, EMBED_DIM), jnp.float32) * row_scale
    table_out = jax.random.normal(key_out, (VOCAB_SIZE, EMBED_DIM), jnp.float32) * row_scale
    return {'table_in': table_in, 'table_out': table_out, 'center_ids': draw_ids(key_center, PAIRS_DEV), 'context_ids': draw_ids(key_context, PAIRS_DEV), 'negative_ids': draw_ids(key_neg, NEGATIVES)}


def reference(table_in, table_out, center_ids, context_ids, negative_ids):
    zero_table = jnp.zeros((VOCAB_SIZE, EMBED_DIM), jnp.float32)

    def scan_body(state_in, batch_ids):
        grad_in, grad_out = state_in
        center_row, context_row, negative_row = batch_ids
        center_vec = jnp.take(table_in, center_row, axis=0)
        context_vec = jnp.take(table_out, context_row, axis=0)
        negative_vec = jnp.take(table_out, negative_row, axis=0)
        pos_score = jnp.sum(center_vec * context_vec, axis=1)
        center_half = center_vec.astype(jnp.bfloat16)
        negative_half = negative_vec.astype(jnp.bfloat16)
        neg_score = jnp.dot(center_half, negative_half.T, preferred_element_type=jnp.float32)
        pos_grad = (jax.nn.sigmoid(pos_score) - 1.0)[:, None]
        neg_grad = (NEG_SCALE * jax.nn.sigmoid(neg_score)).astype(jnp.bfloat16)
        d_center = pos_grad * context_vec + jnp.dot(neg_grad, negative_half, preferred_element_type=jnp.float32)
        d_context = pos_grad * center_vec
        d_negative = jnp.dot(neg_grad.T, center_half, preferred_element_type=jnp.float32)
        grad_in = grad_in.at[center_row].add(d_center)
        grad_out = grad_out.at[context_row].add(d_context).at[negative_row].add(d_negative)
        return (grad_in, grad_out), None

    start_state = (zero_table, zero_table)
    batches = (center_ids.reshape(SHARDS, PAIRS_DEV), context_ids.reshape(SHARDS, PAIRS_DEV), negative_ids.reshape(SHARDS, NEGATIVES))
    grad_in, grad_out = lax.scan(scan_body, start_state, batches)[0]
    return (table_in - LEARN_RATE * grad_in, table_out - LEARN_RATE * grad_out)
```

```python
import functools

import jax
import jax.numpy as jnp
from jax import lax
from jax.experimental import pallas as pl
from jax.sharding import PartitionSpec as P

LEARN_RATE = 1.0
NEG_WEIGHT = 5.0
AXIS_NAME = 'vp'
HOT_ROWS = 768


def unique_capacity(num_ids, shards):
    common_slots = 3 * num_ids // shards
    return common_slots // 4 + (num_ids - common_slots + shards - 1) // shards


def tight_capacity(num_ids, shards):
    return (num_ids - 3 * num_ids // shards + shards - 1) // shards


def running_count(flags):
    lanes = 128
    rows = flags.shape[0] // lanes
    grid = flags.reshape(rows, lanes).astype(jnp.bfloat16)
    upper = (jnp.arange(lanes)[:, None] <= jnp.arange(lanes)[None, :]).astype(jnp.bfloat16)
    inner = jnp.dot(grid, upper, preferred_element_type=jnp.float32)
    lower = (jnp.arange(rows)[:, None] > jnp.arange(rows)[None, :]).astype(jnp.bfloat16)
    outer = jnp.dot(lower, inner[:, -1:].astype(jnp.bfloat16), preferred_element_type=jnp.float32)
    return (inner + outer).astype(jnp.int32).reshape(-1)


def plan_unique(sorted_ids, shard_rows, shards, hot, capacity):
    num_ids = sorted_ids.shape[0]
    previous = jnp.concatenate([jnp.full((1,), -1, jnp.int32), sorted_ids[:-1]])
    first = (sorted_ids != previous) & (sorted_ids >= hot)
    owner = sorted_ids // shard_rows
    rank = running_count(first) - 1
    owners = jnp.arange(shards, dtype=jnp.int32)
    counts = jnp.sum((first[None, :] & (owner[None, :] == owners[:, None])).astype(jnp.int32), axis=1)
    starts = jnp.sum(jnp.where(owners[None, :] < owners[:, None], counts[None, :], 0), axis=1)
    start_of = jnp.sum(jnp.where(owner[:, None] == owners[None, :], starts[None, :], 0), axis=1)
    packed = lax.sort(jnp.where(first, sorted_ids, jnp.int32(2**30)))
    packed = jnp.concatenate([packed, jnp.full((capacity,), 2**30, jnp.int32)])
    asked = jnp.stack([lax.dynamic_slice(packed, (starts[s],), (capacity,)) for s in range(shards)])
    return owner, rank - start_of, asked, jnp.max(counts)


def cell_of(sorted_ids, owner, rank, shards, hot, capacity):
    return jnp.where(sorted_ids < hot, shards * capacity + sorted_ids, owner * capacity + rank)


def round_rows(rows, block=512):
    def body(x_ref, y_ref):
        y_ref[...] = x_ref[...].astype(jnp.bfloat16)

    spec = pl.BlockSpec((block, rows.shape[1]), lambda i: (i, 0))
    return pl.pallas_call(body, grid=(rows.shape[0] // block,), in_specs=[spec], out_specs=spec, out_shape=jax.ShapeDtypeStruct(rows.shape, jnp.bfloat16))(rows)


def exchange(rows, shards):
    return lax.all_to_all(rows.reshape(shards, -1, rows.shape[-1]), AXIS_NAME, 0, 0).reshape(rows.shape)


def solution(mesh):
    shards = mesh.shape[AXIS_NAME]

    def device_step(in_shard, out_shard, center_ids, context_ids, negative_ids):
        shard_rows = in_shard.shape[0]
        num_pairs = center_ids.shape[0]
        num_negs = negative_ids.shape[0]
        hot = HOT_ROWS
        me = lax.axis_index(AXIS_NAME)
        full_pairs, full_negs = unique_capacity(num_pairs, shards), unique_capacity(num_negs, shards)
        tight_pairs, tight_negs = tight_capacity(num_pairs, shards), tight_capacity(num_negs, shards)

        hot_both = jnp.concatenate([in_shard[:hot], out_shard[:hot]])
        hot_both = lax.psum(jnp.where(me == 0, hot_both, 0.0), AXIS_NAME)
        hot_in, hot_out = hot_both[:hot], hot_both[hot:]

        neg_sorted = lax.sort(negative_ids)
        cen_sorted, con_moved = lax.sort((center_ids, context_ids), num_keys=1)
        con_sorted, con_pos = lax.sort((con_moved, jnp.arange(num_pairs, dtype=jnp.int32)), num_keys=1)
        neg_owner, neg_rank, neg_asked, neg_max = plan_unique(neg_sorted, shard_rows, shards, hot, full_negs)
        cen_owner, cen_rank, cen_asked, cen_max = plan_unique(cen_sorted, shard_rows, shards, hot, full_pairs)
        con_owner, con_rank, con_asked, con_max = plan_unique(con_sorted, shard_rows, shards, hot, full_pairs)
        fits = (neg_max <= tight_negs) & (cen_max <= tight_pairs) & (con_max <= tight_pairs)
        spill = jnp.broadcast_to(1 - fits.astype(jnp.int32), (shards, 1))
        asked = lax.all_to_all(jnp.concatenate([neg_asked, cen_asked, con_asked, spill], axis=1), AXIS_NAME, 0, 0)
        all_fit = jnp.sum(asked[:, -1]) == 0
        local = jnp.clip(asked[:, :-1] - me * shard_rows, 0, shard_rows - 1)
        neg_local = local[:, :full_negs]
        cen_local = local[:, full_negs:full_negs + full_pairs]
        con_local = local[:, full_negs + full_pairs:]

        def run(cap_pairs, cap_negs, in_shard, out_shard, hot_in, hot_out, neg_local, cen_local, con_local):
            neg_rows = neg_local[:, :cap_negs].reshape(-1)
            cen_rows = cen_local[:, :cap_pairs].reshape(-1)
            con_rows = con_local[:, :cap_pairs].reshape(-1)
            neg_cell = cell_of(neg_sorted, neg_owner, neg_rank, shards, hot, cap_negs)
            cen_cell = cell_of(cen_sorted, cen_owner, cen_rank, shards, hot, cap_pairs)
            con_cell = cell_of(con_sorted, con_owner, con_rank, shards, hot, cap_pairs)
            con_cell = lax.sort((con_pos, con_cell), num_keys=1)[1]

            take = functools.partial(jnp.take, axis=0, mode='clip')
            neg_got = exchange(take(out_shard, neg_rows), shards)
            cen_send = take(in_shard, cen_rows)
            cen_send, neg_got = lax.optimization_barrier((cen_send, neg_got))
            cen_got = exchange(cen_send, shards)
            con_send = take(out_shard, con_rows)
            con_send, cen_got = lax.optimization_barrier((con_send, cen_got))
            con_got = exchange(con_send, shards)

            negative_half = round_rows(take(jnp.concatenate([neg_got, hot_out]), neg_cell))
            center_vec = take(jnp.concatenate([cen_got, hot_in]), cen_cell)
            center_half = center_vec.astype(jnp.bfloat16)
            neg_scale = NEG_WEIGHT / num_negs
            neg_score = lax.dot_general(center_half, negative_half, (((1,), (1,)), ((), ())), preferred_element_type=jnp.float32)
            neg_grad = (neg_scale * jax.nn.sigmoid(neg_score)).astype(jnp.bfloat16)
            d_negative = lax.dot_general(neg_grad, center_half, (((0,), (0,)), ((), ())), preferred_element_type=jnp.float32)
            neg_sum = jax.ops.segment_sum(d_negative, neg_cell, num_segments=shards * cap_negs + hot, indices_are_sorted=False)
            d_center = jnp.dot(neg_grad, negative_half, preferred_element_type=jnp.float32)

            context_vec = take(jnp.concatenate([con_got, hot_out]), con_cell)
            pos_score = jnp.sum(center_vec * context_vec, axis=1)
            pos_grad = (jax.nn.sigmoid(pos_score) - 1.0)[:, None]
            d_context = pos_grad * center_vec
            con_sum = jax.ops.segment_sum(d_context, con_cell, num_segments=shards * cap_pairs + hot)
            d_center = d_center + pos_grad * context_vec
            cen_sum = jax.ops.segment_sum(d_center, cen_cell, num_segments=shards * cap_pairs + hot)

            neg_back = exchange(neg_sum[:shards * cap_negs], shards)
            con_part = con_sum[:shards * cap_pairs]
            con_part, neg_back = lax.optimization_barrier((con_part, neg_back))
            con_back = exchange(con_part, shards)
            cen_part = cen_sum[:shards * cap_pairs]
            cen_part, con_back = lax.optimization_barrier((cen_part, con_back))
            cen_back = exchange(cen_part, shards)
            out_hot = con_sum[shards * cap_pairs:] + neg_sum[shards * cap_negs:]
            hot_sum = lax.psum(jnp.concatenate([cen_sum[shards * cap_pairs:], out_hot]), AXIS_NAME)
            hot_sum = jnp.where(me == 0, hot_sum, 0.0)

            new_out = out_shard.at[neg_rows].add(-neg_back).at[con_rows].add(-con_back).at[:hot].add(-hot_sum[hot:])
            new_in = in_shard.at[cen_rows].add(-cen_back).at[:hot].add(-hot_sum[:hot])
            return new_in, new_out

        return lax.cond(all_fit, functools.partial(run, tight_pairs, tight_negs), functools.partial(run, full_pairs, full_negs), in_shard, out_shard, hot_in, hot_out, neg_local, cen_local, con_local)

    return jax.shard_map(device_step, mesh=mesh, in_specs=(P(AXIS_NAME, None), P(AXIS_NAME, None), P(AXIS_NAME), P(AXIS_NAME), P(AXIS_NAME)), out_specs=(P(AXIS_NAME, None), P(AXIS_NAME, None)), check_vma=False)
```

```python
import functools

import jax
import jax.numpy as jnp
from jax import lax
from jax.experimental import pallas as pl
from jax.experimental.pallas import tpu as pltpu
from jax.sharding import PartitionSpec as P

LEARN_RATE = 1.0
NEG_WEIGHT = 5.0
AXIS_NAME = 'vp'
HOT_ROWS = 768
LANES = 128
SUBLANES = 8
NO_ID = 2**30
VMEM_BYTES = 60 * 2**20
ANY = pl.BlockSpec(memory_space=pl.ANY)


def unique_capacity(num_ids, shards):
    common_slots = 3 * num_ids // shards
    return common_slots // 4 + (num_ids - common_slots + shards - 1) // shards


def tight_capacity(num_ids, shards):
    return (num_ids - 3 * num_ids // shards + shards - 1) // shards


def tile_view(rows):
    n, d = rows.shape
    return rows.reshape(n // SUBLANES, SUBLANES, d // LANES, LANES).transpose(0, 2, 1, 3).reshape(n * d // LANES, LANES)


def row_view(lines, d):
    n = lines.shape[0] * LANES // d
    return lines.reshape(n // SUBLANES, d // LANES, SUBLANES, LANES).transpose(0, 2, 1, 3).reshape(n, d)


def first_line(row, d):
    return (row // SUBLANES) * (SUBLANES * (d // LANES)) + row % SUBLANES


def gather_rows(table, rows, groups):
    n, d = rows.shape[0], table.shape[1]
    chunks, cap = d // LANES, n // groups
    view = tile_view(table)

    def body(line, t_ref, o_ref):
        group = pl.program_id(0)

        def step(t, carry):
            start = group * cap + t * SUBLANES
            got = [t_ref[pl.ds(line[start + j], chunks, stride=SUBLANES), :] for j in range(SUBLANES)]
            for j in range(SUBLANES):
                o_ref[pl.ds(t * SUBLANES * chunks + j, chunks, stride=SUBLANES), :] = got[j]
            return carry

        lax.fori_loop(0, cap // SUBLANES, step, 0, unroll=4)

    out = pl.pallas_call(
        body,
        grid_spec=pltpu.PrefetchScalarGridSpec(
            num_scalar_prefetch=1, grid=(groups,),
            in_specs=[pl.BlockSpec(view.shape, lambda s, i: (0, 0), pipeline_mode=pl.Buffered(1))],
            out_specs=pl.BlockSpec((cap * chunks, LANES), lambda s, i: (s, 0))),
        out_shape=jax.ShapeDtypeStruct((n * chunks, LANES), table.dtype),
        cost_estimate=pl.CostEstimate(flops=0, bytes_accessed=4 * d * (table.shape[0] + 3 * n), transcendentals=0),
        compiler_params=pltpu.CompilerParams(vmem_limit_bytes=VMEM_BYTES),
        name='gather_rows',
    )(first_line(rows, d), view)
    return row_view(out, d)


def pair_sums(x_hot, x_got, y_hot, y_got, x_row, y_row):
    d = x_hot.shape[1]
    chunks, pairs = d // LANES, x_row.shape[0]
    views = [tile_view(a) for a in (x_hot, x_got, y_hot, y_got)]
    xh_lines, xg_lines, yh_lines, yg_lines = [v.shape[0] for v in views]
    x_lines, y_lines = xh_lines + xg_lines, yh_lines + yg_lines

    def body(x_line, y_line, xh, xg, yh, yg, oh, og, x_all, y_all, total, sem):
        copies = [
            pltpu.make_async_copy(xh, x_all.at[pl.ds(0, xh_lines)], sem.at[0]),
            pltpu.make_async_copy(xg, x_all.at[pl.ds(xh_lines, xg_lines)], sem.at[1]),
            pltpu.make_async_copy(yh, y_all.at[pl.ds(0, yh_lines)], sem.at[2]),
            pltpu.make_async_copy(yg, y_all.at[pl.ds(yh_lines, yg_lines)], sem.at[3]),
        ]
        for copy in copies:
            copy.start()

        def zero(t, carry):
            total[pl.ds(pl.multiple_of(t * 64, 64), 64), :] = jnp.zeros((64, LANES), jnp.float32)
            return carry

        lax.fori_loop(0, y_lines // 64, zero, 0)
        for copy in copies:
            copy.wait()

        def step(t, carry):
            run, last = carry
            kept, parts, lines = [], [], []
            for j in range(SUBLANES):
                line = y_line[t * SUBLANES + j]
                x = x_all[pl.ds(x_line[t * SUBLANES + j], chunks, stride=SUBLANES), :]
                y = y_all[pl.ds(line, chunks, stride=SUBLANES), :]
                kept.append(x)
                lines.append(line)
                parts.append(jnp.sum(x * y, axis=0, keepdims=True))
            score = jnp.sum(jnp.concatenate(parts, axis=0), axis=1, keepdims=True)
            grad = jax.nn.sigmoid(score) - 1.0
            for j in range(SUBLANES):
                same = (lines[j] == last).astype(jnp.float32)
                run = run * same + grad[j:j + 1, :] * kept[j]
                total[pl.ds(lines[j], chunks, stride=SUBLANES), :] = run
                last = lines[j]
            return run, last

        lax.fori_loop(0, pairs // SUBLANES, step, (jnp.zeros((chunks, LANES), jnp.float32), jnp.int32(-1)), unroll=2)
        out_hot = pltpu.make_async_copy(total.at[pl.ds(0, yh_lines)], oh, sem.at[0])
        out_got = pltpu.make_async_copy(total.at[pl.ds(yh_lines, yg_lines)], og, sem.at[1])
        out_hot.start()
        out_got.start()
        out_hot.wait()
        out_got.wait()

    oh, og = pl.pallas_call(
        body,
        grid_spec=pltpu.PrefetchScalarGridSpec(
            num_scalar_prefetch=2, grid=(1,), in_specs=[ANY] * 4, out_specs=[ANY] * 2,
            scratch_shapes=[pltpu.VMEM((x_lines, LANES), jnp.float32), pltpu.VMEM((y_lines, LANES), jnp.float32),
                            pltpu.VMEM((y_lines, LANES), jnp.float32), pltpu.SemaphoreType.DMA((4,))]),
        out_shape=[jax.ShapeDtypeStruct((yh_lines, LANES), jnp.float32), jax.ShapeDtypeStruct((yg_lines, LANES), jnp.float32)],
        cost_estimate=pl.CostEstimate(flops=0, bytes_accessed=8 * 4 * d * pairs, transcendentals=0),
        compiler_params=pltpu.CompilerParams(vmem_limit_bytes=VMEM_BYTES),
        name='pair_sums',
    )(first_line(x_row, d), first_line(y_row, d), *views)
    return row_view(oh, d), row_view(og, d)


def subtract_rows(table, hot, parts):
    d = table.shape[1]
    chunks, batch = d // LANES, 16
    groups = parts[0][0].shape[0]
    caps = [rows.shape[1] for rows, _ in parts]
    view, hot_view = tile_view(table), tile_view(hot)
    lines = view.shape[0]
    count = len(parts)

    def body(*refs):
        line = refs[:count]
        t_hbm, h_ref = refs[count:count + 2]
        values = refs[count + 2:2 * count + 2]
        o_hbm, held, sem = refs[2 * count + 2:]
        group = pl.program_id(0)

        @pl.when(group == 0)
        def _():
            copy = pltpu.make_async_copy(t_hbm, held.at[pl.ds(0, lines)], sem)
            copy.start()
            copy.wait()

            def hot_step(t, carry):
                window = pl.ds(pl.multiple_of(t * 64, 64), 64)
                held[window, :] = held[window, :] - LEARN_RATE * h_ref[window, :]
                return carry

            lax.fori_loop(0, h_ref.shape[0] // 64, hot_step, 0)

        for p in range(count):
            def step(t, carry, p=p):
                at = [line[p][group * caps[p] + t * batch + j] for j in range(batch)]
                new = []
                for j in range(batch):
                    source = (t * (batch // SUBLANES) + j // SUBLANES) * SUBLANES * chunks + j % SUBLANES
                    value = values[p][pl.ds(source, chunks, stride=SUBLANES), :]
                    new.append(held[pl.ds(at[j], chunks, stride=SUBLANES), :] - LEARN_RATE * value)
                for j in range(batch):
                    held[pl.ds(at[j], chunks, stride=SUBLANES), :] = new[j]
                return carry

            lax.fori_loop(0, caps[p] // batch, step, 0)

        @pl.when(group == groups - 1)
        def _():
            copy = pltpu.make_async_copy(held.at[pl.ds(0, lines)], o_hbm, sem)
            copy.start()
            copy.wait()

    out = pl.pallas_call(
        body,
        grid_spec=pltpu.PrefetchScalarGridSpec(
            num_scalar_prefetch=count, grid=(groups,),
            in_specs=[ANY, pl.BlockSpec(hot_view.shape, lambda s, *i: (0, 0))] + [pl.BlockSpec((c * chunks, LANES), lambda s, *i: (s, 0)) for c in caps],
            out_specs=ANY,
            scratch_shapes=[pltpu.VMEM((lines + SUBLANES * chunks, LANES), jnp.float32), pltpu.SemaphoreType.DMA]),
        out_shape=jax.ShapeDtypeStruct((lines, LANES), jnp.float32),
        cost_estimate=pl.CostEstimate(flops=0, bytes_accessed=4 * d * (2 * table.shape[0] + 3 * groups * sum(caps)), transcendentals=0),
        compiler_params=pltpu.CompilerParams(vmem_limit_bytes=VMEM_BYTES),
        name='subtract_rows',
    )(*[first_line(rows.reshape(-1), d) for rows, _ in parts], view, hot_view, *[tile_view(values) for _, values in parts])
    return row_view(out, d)


def split_rows(sources, times, block=256):
    d = sources[0].shape[1]
    blocks = [a.shape[0] // block for a in sources]
    starts = [sum(blocks[:k]) for k in range(len(blocks))]
    total = sum(blocks) * block

    def body(*refs):
        ins, t_ref, (r_ref, h_ref, l_ref) = refs[:len(sources)], refs[len(sources)], refs[len(sources) + 1:]
        step = pl.program_id(0)
        for k, ref in enumerate(ins):
            @pl.when((step >= starts[k]) & (step < starts[k] + blocks[k]))
            def _(ref=ref):
                rounded = ref[...].astype(jnp.bfloat16)
                scaled = rounded.astype(jnp.float32) * t_ref[...]
                high = scaled.astype(jnp.bfloat16)
                r_ref[...] = rounded
                h_ref[...] = high
                l_ref[...] = (scaled - high.astype(jnp.float32)).astype(jnp.bfloat16)

    def pick(k):
        return lambda i: (jnp.clip(i - starts[k], 0, blocks[k] - 1), 0)

    spec = pl.BlockSpec((block, d), lambda i: (i, 0))
    return pl.pallas_call(
        body, grid=(sum(blocks),),
        in_specs=[pl.BlockSpec((block, d), pick(k)) for k in range(len(sources))] + [pl.BlockSpec((block, 1), lambda i: (i, 0))],
        out_specs=[spec] * 3, out_shape=[jax.ShapeDtypeStruct((total, d), jnp.bfloat16)] * 3,
        cost_estimate=pl.CostEstimate(flops=0, bytes_accessed=10 * d * total, transcendentals=0),
        name='split_rows',
    )(*sources, times.astype(jnp.float32)[:, None])


def running_count(flags):
    rows = flags.shape[0] // LANES
    grid = flags.reshape(rows, LANES).astype(jnp.bfloat16)
    upper = (jnp.arange(LANES)[:, None] <= jnp.arange(LANES)[None, :]).astype(jnp.bfloat16)
    inner = jnp.dot(grid, upper, preferred_element_type=jnp.float32)
    lower = (jnp.arange(rows)[:, None] > jnp.arange(rows)[None, :]).astype(jnp.bfloat16)
    outer = jnp.dot(lower, inner[:, -1:].astype(jnp.bfloat16), preferred_element_type=jnp.float32)
    return (inner + outer).astype(jnp.int32).reshape(-1)


def mark_unique(sorted_ids, shard_rows, shards, hot):
    previous = jnp.concatenate([jnp.full((1,), -1, jnp.int32), sorted_ids[:-1]])
    first = (sorted_ids != previous) & (sorted_ids >= hot)
    owner = sorted_ids // shard_rows
    rank = running_count(first) - 1
    owners = jnp.arange(shards, dtype=jnp.int32)
    counts = jnp.sum((first[None, :] & (owner[None, :] == owners[:, None])).astype(jnp.int32), axis=1)
    starts = jnp.sum(jnp.where(owners[None, :] < owners[:, None], counts[None, :], 0), axis=1)
    start_of = jnp.sum(jnp.where(owner[None, :] == owners[:, None], starts[:, None], 0), axis=0)
    return first, owner, rank - start_of, counts, starts


def cut_lists(packed, starts, capacity):
    padded = jnp.concatenate([packed, jnp.full((capacity,), packed.shape[0], jnp.int32)])
    return jnp.stack([lax.dynamic_slice(padded, (starts[s],), (capacity,)) for s in range(starts.shape[0])])


def ask_lists(sorted_ids, first, counts, starts, shard_rows, shards, capacity):
    num_ids = sorted_ids.shape[0]
    place = jnp.where(first, jnp.arange(num_ids, dtype=jnp.int32), num_ids)
    packed, places = lax.sort((jnp.where(first, sorted_ids, NO_ID), place), num_keys=1)
    valid = jnp.arange(capacity, dtype=jnp.int32)[None, :] < counts[:, None]
    past = (jnp.arange(shards, dtype=jnp.int32)[:, None] + 1) * shard_rows
    asked = jnp.where(valid, cut_lists(packed, starts, capacity), past)
    after = jnp.concatenate([places[1:], jnp.full((1,), num_ids, jnp.int32)])
    times = jnp.where(valid, cut_lists(after - places, starts, capacity), 0)
    return asked, times.reshape(-1)


def hot_times(ids, hot):
    return jnp.sum((ids[None, :] == jnp.arange(hot, dtype=jnp.int32)[:, None]).astype(jnp.int32), axis=1)


def cell_of(sorted_ids, owner, rank, shards, hot, capacity):
    return jnp.where(sorted_ids < hot, sorted_ids, jnp.minimum(hot + owner * capacity + rank, hot + shards * capacity - 1))


def exchange(rows, shards):
    return lax.all_to_all(rows.reshape(shards, -1, rows.shape[-1]), AXIS_NAME, 0, 0).reshape(rows.shape)


def exchange_ids(ids):
    return lax.all_to_all(ids, AXIS_NAME, 0, 0)


def dot(a, b, dims):
    return lax.dot_general(a, b, (dims, ((), ())), preferred_element_type=jnp.float32)


def after(value, earlier):
    return lax.optimization_barrier((value, earlier))


def when(predicate, update, value):
    return lax.while_loop(lambda state: state[0], lambda state: (jnp.zeros((), jnp.bool_), update(state[1])), (predicate, value))[1]


def plan_unique(sorted_ids, shard_rows, shards, capacity):
    num_ids = sorted_ids.shape[0]
    previous = jnp.concatenate([jnp.full((1,), -1, jnp.int32), sorted_ids[:-1]])
    first = (sorted_ids != previous)
    owner = sorted_ids // shard_rows
    rank = running_count(first) - 1
    owners = jnp.arange(shards, dtype=jnp.int32)
    counts = jnp.sum((first[None, :] & (owner[None, :] == owners[:, None])).astype(jnp.int32), axis=1)
    starts = jnp.sum(jnp.where(owners[None, :] < owners[:, None], counts[None, :], 0), axis=1)
    start_of = jnp.sum(jnp.where(owner[:, None] == owners[None, :], starts[None, :], 0), axis=1)
    packed = lax.sort(jnp.where(first, sorted_ids, jnp.int32(NO_ID)))
    packed = jnp.concatenate([packed, jnp.full((capacity,), NO_ID, jnp.int32)])
    asked = jnp.stack([lax.dynamic_slice(packed, (starts[s],), (capacity,)) for s in range(shards)])
    return owner, rank - start_of, asked


def full_step(shards, in_shard, out_shard, center_ids, context_ids, negative_ids):
    shard_rows = in_shard.shape[0]
    num_pairs, num_negs = center_ids.shape[0], negative_ids.shape[0]
    cap_pairs, cap_negs = unique_capacity(num_pairs, shards), unique_capacity(num_negs, shards)
    me = lax.axis_index(AXIS_NAME)
    take = functools.partial(jnp.take, axis=0, mode='clip')
    neg_sorted = lax.sort(negative_ids)
    cen_sorted, con_moved = lax.sort((center_ids, context_ids), num_keys=1)
    con_sorted, con_pos = lax.sort((con_moved, jnp.arange(num_pairs, dtype=jnp.int32)), num_keys=1)

    def fetch(table, sorted_ids, capacity):
        owner, rank, asked = plan_unique(sorted_ids, shard_rows, shards, capacity)
        local = jnp.clip(exchange_ids(asked) - me * shard_rows, 0, shard_rows - 1).reshape(-1)
        return owner * capacity + rank, local, exchange(take(table, local), shards)

    neg_cell, neg_local, neg_got = fetch(out_shard, neg_sorted, cap_negs)
    cen_cell, cen_local, cen_got = fetch(in_shard, cen_sorted, cap_pairs)
    con_cell, con_local, con_got = fetch(out_shard, con_sorted, cap_pairs)
    con_cell = lax.sort((con_pos, con_cell), num_keys=1)[1]
    negative_half = split_rows([take(neg_got, neg_cell)], jnp.ones((num_negs,), jnp.float32))[0]
    center_vec = take(cen_got, cen_cell)
    center_half = split_rows([center_vec], jnp.ones((num_pairs,), jnp.float32))[0]
    neg_grad = (NEG_WEIGHT / num_negs * jax.nn.sigmoid(dot(center_half, negative_half, ((1,), (1,))))).astype(jnp.bfloat16)
    context_vec = take(con_got, con_cell)
    pos_grad = (jax.nn.sigmoid(jnp.sum(center_vec * context_vec, axis=1)) - 1.0)[:, None]
    d_center = dot(neg_grad, negative_half, ((1,), (0,))) + pos_grad * context_vec
    d_negative = dot(neg_grad, center_half, ((0,), (0,)))

    def give(table, grads, cell, local, capacity):
        sums = jax.ops.segment_sum(grads, cell, num_segments=shards * capacity)
        return table.at[local].add(-LEARN_RATE * exchange(sums, shards))

    new_out = give(out_shard, d_negative, neg_cell, neg_local, cap_negs)
    new_out = give(new_out, pos_grad * center_vec, con_cell, con_local, cap_pairs)
    return give(in_shard, d_center, cen_cell, cen_local, cap_pairs), new_out


def tight_step(shards, in_shard, out_shard, center_ids, context_ids, negative_ids):
    shard_rows = in_shard.shape[0]
    num_pairs, num_negs = center_ids.shape[0], negative_ids.shape[0]
    hot = HOT_ROWS
    cap_pairs, cap_negs = tight_capacity(num_pairs, shards), tight_capacity(num_negs, shards)
    me = lax.axis_index(AXIS_NAME)

    hot_both = jnp.concatenate([in_shard[:hot], out_shard[:hot]])
    hot_both = lax.psum(jnp.where(me == 0, hot_both, 0.0), AXIS_NAME)
    hot_in, hot_out = hot_both[:hot], hot_both[hot:]

    neg_sorted = lax.sort(negative_ids)
    neg_first, _, _, neg_counts, neg_starts = mark_unique(neg_sorted, shard_rows, shards, hot)
    neg_asked, neg_times = ask_lists(neg_sorted, neg_first, neg_counts, neg_starts, shard_rows, shards, cap_negs)
    neg_local = exchange_ids(neg_asked) - me * shard_rows
    neg_send = gather_rows(out_shard, jnp.minimum(neg_local, shard_rows - 1).reshape(-1), shards)
    neg_got = exchange(neg_send, shards)

    cen_sorted, con_moved = lax.sort((center_ids, context_ids), num_keys=1)
    cen_first, cen_owner, cen_rank, cen_counts, cen_starts = mark_unique(cen_sorted, shard_rows, shards, hot)
    cen_asked, cen_times = ask_lists(cen_sorted, cen_first, cen_counts, cen_starts, shard_rows, shards, cap_pairs)
    cen_cell = cell_of(cen_sorted, cen_owner, cen_rank, shards, hot, cap_pairs)
    con_sorted, cen_by_con = lax.sort((con_moved, cen_cell), num_keys=1)
    con_first, con_owner, con_rank, con_counts, con_starts = mark_unique(con_sorted, shard_rows, shards, hot)
    con_asked, _ = ask_lists(con_sorted, con_first, con_counts, con_starts, shard_rows, shards, cap_pairs)
    con_cell = cell_of(con_sorted, con_owner, con_rank, shards, hot, cap_pairs)
    fits = (jnp.max(neg_counts) <= cap_negs) & (jnp.max(cen_counts) <= cap_pairs) & (jnp.max(con_counts) <= cap_pairs)
    spill = jnp.broadcast_to(1 - fits.astype(jnp.int32), (shards, 1))
    asked = exchange_ids(jnp.concatenate([cen_asked, con_asked, spill], axis=1))
    all_fit = jnp.sum(asked[:, -1]) == 0
    cen_local = asked[:, :cap_pairs] - me * shard_rows
    con_local = asked[:, cap_pairs:2 * cap_pairs] - me * shard_rows
    cen_order, con_by_cen = lax.sort((cen_by_con, con_cell), num_keys=1)

    cen_send = gather_rows(in_shard, jnp.minimum(cen_local, shard_rows - 1).reshape(-1), shards)
    cen_send, neg_got = after(cen_send, neg_got)
    cen_got = exchange(cen_send, shards)
    con_send = gather_rows(out_shard, jnp.minimum(con_local, shard_rows - 1).reshape(-1), shards)
    con_send, cen_got = after(con_send, cen_got)
    con_got = exchange(con_send, shards)

    neg_times = jnp.concatenate([hot_times(negative_ids, hot), neg_times])
    hot_cen_times = hot_times(center_ids, hot)
    w_half, w_high, w_low = split_rows([hot_out, neg_got], neg_times)
    uh_half, uh_high, uh_low = split_rows([hot_in], hot_cen_times)
    uc_half, uc_high, uc_low = split_rows([cen_got], cen_times)

    def neg_grads(u_half):
        return (NEG_WEIGHT / num_negs * jax.nn.sigmoid(dot(u_half, w_half, ((1,), (1,))))).astype(jnp.bfloat16)

    grad_h, grad_c = neg_grads(uh_half), neg_grads(uc_half)
    rows_in, cols_in = ((0,), (0,)), ((1,), (0,))

    def rest(times, half, high, low):
        return (times.astype(jnp.float32)[:, None] * half.astype(jnp.float32) - high.astype(jnp.float32) - low.astype(jnp.float32)).astype(jnp.bfloat16)

    d_neg = dot(grad_h, uh_high, rows_in) + dot(grad_h, uh_low, rows_in) + dot(grad_c, uc_high, rows_in)
    more = (jnp.max(cen_times) > 2) | (jnp.max(hot_cen_times) > 256)
    d_neg = when(more, lambda d: d + dot(grad_c, uc_low, rows_in) + dot(grad_h, rest(hot_cen_times, uh_half, uh_high, uh_low), rows_in) + dot(grad_c, rest(cen_times, uc_half, uc_high, uc_low), rows_in), d_neg)
    d_neg = jnp.where(neg_times[:, None] > 0, neg_times.astype(jnp.float32)[:, None] * d_neg, 0.0)
    neg_part, neg_hot = d_neg[hot:], d_neg[:hot]

    con_hot, con_part = pair_sums(hot_in, cen_got, hot_out, con_got, cen_by_con, con_cell)
    cen_hot, cen_part = pair_sums(hot_out, con_got, hot_in, cen_got, con_by_cen, cen_order)

    def center_grads(grad, times, pair_part):
        d = dot(grad, w_high, cols_in) + dot(grad[:, :hot], w_low[:hot], cols_in)
        more = (jnp.max(neg_times[hot:]) > 2) | (jnp.max(neg_times) > 256)
        d = when(more, lambda d: d + dot(grad[:, hot:], w_low[hot:], cols_in) + dot(grad, rest(neg_times, w_half, w_high, w_low), cols_in), d)
        return jnp.where(times[:, None] > 0, times.astype(jnp.float32)[:, None] * d + pair_part, 0.0)

    cen_hot = center_grads(grad_h, hot_cen_times, cen_hot)
    cen_part = center_grads(grad_c, cen_times, cen_part)

    neg_part, con_got = after(neg_part, con_got)
    neg_back = exchange(neg_part, shards)
    con_part, neg_back = after(con_part, neg_back)
    con_back = exchange(con_part, shards)
    cen_part, con_back = after(cen_part, con_back)
    cen_back = exchange(cen_part, shards)
    out_hot = jnp.where(me == 0, lax.psum(con_hot + neg_hot, AXIS_NAME), 0.0)
    in_hot = jnp.where(me == 0, lax.psum(cen_hot, AXIS_NAME), 0.0)
    new_out = subtract_rows(out_shard, out_hot, [(neg_local, neg_back), (con_local, con_back)])
    new_in = subtract_rows(in_shard, in_hot, [(cen_local, cen_back)])
    return new_in, new_out, all_fit


def solution(mesh):
    shards = mesh.shape[AXIS_NAME]

    def device_step(*args):
        new_in, new_out, all_fit = tight_step(shards, *args)
        return when(~all_fit, lambda _: full_step(shards, *args), (new_in, new_out))

    return jax.shard_map(device_step, mesh=mesh, in_specs=(P(AXIS_NAME, None), P(AXIS_NAME, None), P(AXIS_NAME), P(AXIS_NAME), P(AXIS_NAME)), out_specs=(P(AXIS_NAME, None), P(AXIS_NAME, None)), check_vma=False)
```

```python
import functools

import jax
import jax.numpy as jnp
from jax import lax
from jax.experimental import pallas as pl
from jax.experimental.pallas import tpu as pltpu
from jax.sharding import PartitionSpec as P


LEARN_RATE = 1.0
NEG_WEIGHT = 5.0
AXIS_NAME = 'vp'
HOT_ROWS = 768
LANES = 128
SUBLANES = 8
PAIR_TILES = 4
NO_ID = 2**30
VMEM_BYTES = 60 * 2**20
ANY = pl.BlockSpec(memory_space=pl.ANY)


def unique_capacity(num_ids, shards):
    common_slots = 3 * num_ids // shards
    return common_slots // 4 + (num_ids - common_slots + shards - 1) // shards


def tight_capacity(num_ids, shards):
    return (num_ids - 3 * num_ids // shards + shards - 1) // shards


def tile_view(rows):
    n, d = rows.shape
    return rows.reshape(n // SUBLANES, SUBLANES, d // LANES, LANES).transpose(0, 2, 1, 3).reshape(n * d // LANES, LANES)


def row_view(lines, d):
    n = lines.shape[0] * LANES // d
    return lines.reshape(n // SUBLANES, d // LANES, SUBLANES, LANES).transpose(0, 2, 1, 3).reshape(n, d)


def first_line(row, d):
    return (row // SUBLANES) * (SUBLANES * (d // LANES)) + row % SUBLANES


def gather_rows(table, rows, groups):
    n, d = rows.shape[0], table.shape[1]
    chunks, cap = d // LANES, n // groups
    view = tile_view(table)

    def body(line, t_ref, o_ref):
        group = pl.program_id(0)

        def step(t, carry):
            start = group * cap + t * SUBLANES
            got = [t_ref[pl.ds(line[start + j], chunks, stride=SUBLANES), :] for j in range(SUBLANES)]
            for j in range(SUBLANES):
                o_ref[pl.ds(t * SUBLANES * chunks + j, chunks, stride=SUBLANES), :] = got[j]
            return carry

        lax.fori_loop(0, cap // SUBLANES, step, 0, unroll=4)

    out = pl.pallas_call(
        body,
        grid_spec=pltpu.PrefetchScalarGridSpec(
            num_scalar_prefetch=1, grid=(groups,),
            in_specs=[pl.BlockSpec(view.shape, lambda s, i: (0, 0), pipeline_mode=pl.Buffered(1))],
            out_specs=pl.BlockSpec((cap * chunks, LANES), lambda s, i: (s, 0))),
        out_shape=jax.ShapeDtypeStruct((n * chunks, LANES), table.dtype),
        cost_estimate=pl.CostEstimate(flops=0, bytes_accessed=4 * d * (table.shape[0] + 3 * n), transcendentals=0),
        compiler_params=pltpu.CompilerParams(vmem_limit_bytes=VMEM_BYTES),
        name='gather_rows',
    )(first_line(rows, d), view)
    return row_view(out, d)


def pair_sums(x_hot, x_got, y_hot, y_got, x_row, y_row):
    d = x_hot.shape[1]
    chunks, pairs = d // LANES, x_row.shape[0]
    views = [tile_view(a) for a in (x_hot, x_got, y_hot, y_got)]
    xh_lines, xg_lines, yh_lines, yg_lines = [v.shape[0] for v in views]
    x_lines, y_lines = xh_lines + xg_lines, yh_lines + yg_lines

    def body(x_line, y_line, xh, xg, yh, yg, oh, og, x_all, y_all, total, prod, sem):
        copies = [
            pltpu.make_async_copy(xh, x_all.at[pl.ds(0, xh_lines)], sem.at[0]),
            pltpu.make_async_copy(xg, x_all.at[pl.ds(xh_lines, xg_lines)], sem.at[1]),
            pltpu.make_async_copy(yh, y_all.at[pl.ds(0, yh_lines)], sem.at[2]),
            pltpu.make_async_copy(yg, y_all.at[pl.ds(yh_lines, yg_lines)], sem.at[3]),
        ]
        for copy in copies:
            copy.start()

        def zero(t, carry):
            total[pl.ds(pl.multiple_of(t * 64, 64), 64), :] = jnp.zeros((64, LANES), jnp.float32)
            return carry

        lax.fori_loop(0, y_lines // 64, zero, 0)
        for copy in copies:
            copy.wait()

        def step(t, carry):
            run, last = carry
            kept, lines, grads = [], [], []
            for i in range(PAIR_TILES * SUBLANES):
                tile, j = i // SUBLANES, i % SUBLANES
                line = y_line[t * PAIR_TILES * SUBLANES + i]
                x = x_all[pl.ds(x_line[t * PAIR_TILES * SUBLANES + i], chunks, stride=SUBLANES), :]
                y = y_all[pl.ds(line, chunks, stride=SUBLANES), :]
                prod[pl.ds(tile * SUBLANES * chunks + j, chunks, stride=SUBLANES), :] = x * y
                kept.append(x)
                lines.append(line)
            for tile in range(PAIR_TILES):
                part = prod[pl.ds(tile * SUBLANES * chunks, SUBLANES), :]
                for k in range(1, chunks):
                    part = part + prod[pl.ds((tile * chunks + k) * SUBLANES, SUBLANES), :]
                score = jnp.broadcast_to(jnp.sum(part, axis=1, keepdims=True), (SUBLANES, LANES))
                grads.append(jax.nn.sigmoid(score) - 1.0)
            for i in range(PAIR_TILES * SUBLANES):
                tile, j = i // SUBLANES, i % SUBLANES
                same = (lines[i] == last).astype(jnp.float32)
                run = run * same + jnp.broadcast_to(grads[tile][j:j + 1, :], (chunks, LANES)) * kept[i]
                total[pl.ds(lines[i], chunks, stride=SUBLANES), :] = run
                last = lines[i]
            return run, last

        lax.fori_loop(0, pairs // (PAIR_TILES * SUBLANES), step, (jnp.zeros((chunks, LANES), jnp.float32), jnp.int32(-1)))
        out_hot = pltpu.make_async_copy(total.at[pl.ds(0, yh_lines)], oh, sem.at[0])
        out_got = pltpu.make_async_copy(total.at[pl.ds(yh_lines, yg_lines)], og, sem.at[1])
        out_hot.start()
        out_got.start()
        out_hot.wait()
        out_got.wait()

    oh, og = pl.pallas_call(
        body,
        grid_spec=pltpu.PrefetchScalarGridSpec(
            num_scalar_prefetch=2, grid=(1,), in_specs=[ANY] * 4, out_specs=[ANY] * 2,
            scratch_shapes=[pltpu.VMEM((x_lines, LANES), jnp.float32), pltpu.VMEM((y_lines, LANES), jnp.float32),
                            pltpu.VMEM((y_lines, LANES), jnp.float32), pltpu.VMEM((PAIR_TILES * SUBLANES * chunks, LANES), jnp.float32),
                            pltpu.SemaphoreType.DMA((4,))]),
        out_shape=[jax.ShapeDtypeStruct((yh_lines, LANES), jnp.float32), jax.ShapeDtypeStruct((yg_lines, LANES), jnp.float32)],
        cost_estimate=pl.CostEstimate(flops=0, bytes_accessed=8 * 4 * d * pairs, transcendentals=0),
        compiler_params=pltpu.CompilerParams(vmem_limit_bytes=VMEM_BYTES),
        name='pair_sums',
    )(first_line(x_row, d), first_line(y_row, d), *views)
    return row_view(oh, d), row_view(og, d)


def subtract_rows(table, hot, parts):
    d = table.shape[1]
    chunks, batch = d // LANES, 16
    groups = parts[0][0].shape[0]
    caps = [rows.shape[1] for rows, _ in parts]
    view, hot_view = tile_view(table), tile_view(hot)
    lines = view.shape[0]
    count = len(parts)

    def body(*refs):
        line = refs[:count]
        t_hbm, h_ref = refs[count:count + 2]
        values = refs[count + 2:2 * count + 2]
        o_hbm, held, sem = refs[2 * count + 2:]
        group = pl.program_id(0)

        @pl.when(group == 0)
        def _():
            copy = pltpu.make_async_copy(t_hbm, held.at[pl.ds(0, lines)], sem)
            copy.start()
            copy.wait()

            def hot_step(t, carry):
                window = pl.ds(pl.multiple_of(t * 64, 64), 64)
                held[window, :] = held[window, :] - LEARN_RATE * h_ref[window, :]
                return carry

            lax.fori_loop(0, h_ref.shape[0] // 64, hot_step, 0)

        for p in range(count):
            def step(t, carry, p=p):
                at = [line[p][group * caps[p] + t * batch + j] for j in range(batch)]
                new = []
                for j in range(batch):
                    source = (t * (batch // SUBLANES) + j // SUBLANES) * SUBLANES * chunks + j % SUBLANES
                    value = values[p][pl.ds(source, chunks, stride=SUBLANES), :]
                    new.append(held[pl.ds(at[j], chunks, stride=SUBLANES), :] - LEARN_RATE * value)
                for j in range(batch):
                    held[pl.ds(at[j], chunks, stride=SUBLANES), :] = new[j]
                return carry

            lax.fori_loop(0, caps[p] // batch, step, 0)

        @pl.when(group == groups - 1)
        def _():
            copy = pltpu.make_async_copy(held.at[pl.ds(0, lines)], o_hbm, sem)
            copy.start()
            copy.wait()

    out = pl.pallas_call(
        body,
        grid_spec=pltpu.PrefetchScalarGridSpec(
            num_scalar_prefetch=count, grid=(groups,),
            in_specs=[ANY, pl.BlockSpec(hot_view.shape, lambda s, *i: (0, 0))] + [pl.BlockSpec((c * chunks, LANES), lambda s, *i: (s, 0)) for c in caps],
            out_specs=ANY,
            scratch_shapes=[pltpu.VMEM((lines + SUBLANES * chunks, LANES), jnp.float32), pltpu.SemaphoreType.DMA]),
        out_shape=jax.ShapeDtypeStruct((lines, LANES), jnp.float32),
        cost_estimate=pl.CostEstimate(flops=0, bytes_accessed=4 * d * (2 * table.shape[0] + 3 * groups * sum(caps)), transcendentals=0),
        compiler_params=pltpu.CompilerParams(vmem_limit_bytes=VMEM_BYTES),
        name='subtract_rows',
    )(*[first_line(rows.reshape(-1), d) for rows, _ in parts], view, hot_view, *[tile_view(values) for _, values in parts])
    return row_view(out, d)


def split_rows(sources, times, block=256):
    d = sources[0].shape[1]
    blocks = [a.shape[0] // block for a in sources]
    starts = [sum(blocks[:k]) for k in range(len(blocks))]
    total = sum(blocks) * block

    def body(*refs):
        ins, t_ref, (r_ref, h_ref, l_ref) = refs[:len(sources)], refs[len(sources)], refs[len(sources) + 1:]
        step = pl.program_id(0)
        for k, ref in enumerate(ins):
            @pl.when((step >= starts[k]) & (step < starts[k] + blocks[k]))
            def _(ref=ref):
                rounded = ref[...].astype(jnp.bfloat16)
                scaled = rounded.astype(jnp.float32) * t_ref[...]
                high = scaled.astype(jnp.bfloat16)
                r_ref[...] = rounded
                h_ref[...] = high
                l_ref[...] = (scaled - high.astype(jnp.float32)).astype(jnp.bfloat16)

    def pick(k):
        return lambda i: (jnp.clip(i - starts[k], 0, blocks[k] - 1), 0)

    spec = pl.BlockSpec((block, d), lambda i: (i, 0))
    return pl.pallas_call(
        body, grid=(sum(blocks),),
        in_specs=[pl.BlockSpec((block, d), pick(k)) for k in range(len(sources))] + [pl.BlockSpec((block, 1), lambda i: (i, 0))],
        out_specs=[spec] * 3, out_shape=[jax.ShapeDtypeStruct((total, d), jnp.bfloat16)] * 3,
        cost_estimate=pl.CostEstimate(flops=0, bytes_accessed=10 * d * total, transcendentals=0),
        name='split_rows',
    )(*sources, times.astype(jnp.float32)[:, None])


def running_count(flags):
    rows = flags.shape[0] // LANES
    grid = flags.reshape(rows, LANES).astype(jnp.bfloat16)
    upper = (jnp.arange(LANES)[:, None] <= jnp.arange(LANES)[None, :]).astype(jnp.bfloat16)
    inner = jnp.dot(grid, upper, preferred_element_type=jnp.float32)
    lower = (jnp.arange(rows)[:, None] > jnp.arange(rows)[None, :]).astype(jnp.bfloat16)
    outer = jnp.dot(lower, inner[:, -1:].astype(jnp.bfloat16), preferred_element_type=jnp.float32)
    return (inner + outer).astype(jnp.int32).reshape(-1)


def mark_unique(sorted_ids, shard_rows, shards, hot):
    previous = jnp.concatenate([jnp.full((1,), -1, jnp.int32), sorted_ids[:-1]])
    first = (sorted_ids != previous) & (sorted_ids >= hot)
    owner = sorted_ids // shard_rows
    rank = running_count(first) - 1
    owners = jnp.arange(shards, dtype=jnp.int32)
    counts = jnp.sum((first[None, :] & (owner[None, :] == owners[:, None])).astype(jnp.int32), axis=1)
    starts = jnp.sum(jnp.where(owners[None, :] < owners[:, None], counts[None, :], 0), axis=1)
    start_of = jnp.sum(jnp.where(owner[None, :] == owners[:, None], starts[:, None], 0), axis=0)
    return first, owner, rank - start_of, counts


def ask_lists(sorted_ids, first, owner, rank, counts, shard_rows, shards, capacity):
    num_ids = sorted_ids.shape[0]
    cells = shards * capacity
    key = jnp.where(first & (rank < capacity), owner * capacity + rank, NO_ID)
    owners = jnp.arange(shards, dtype=jnp.int32)[:, None]
    slot = jnp.arange(capacity, dtype=jnp.int32)[None, :]
    past = (owners + 1) * shard_rows
    ends = jnp.sum((sorted_ids[None, :] < past).astype(jnp.int32), axis=1, keepdims=True)
    fill_key = jnp.where(slot >= counts[:, None], owners * capacity + slot, NO_ID)

    def flat(values):
        return jnp.broadcast_to(values, (shards, capacity)).reshape(-1)

    _, asked, places = lax.sort((
        jnp.concatenate([key, fill_key.reshape(-1)]),
        jnp.concatenate([sorted_ids, flat(past)]),
        jnp.concatenate([jnp.arange(num_ids, dtype=jnp.int32), flat(ends)])), num_keys=1)
    places = places[:cells]
    times = jnp.concatenate([places[1:], jnp.full((1,), num_ids, jnp.int32)]) - places
    return asked[:cells].reshape(shards, capacity), times


def hot_times(ids, hot):
    return jnp.sum((ids[None, :] == jnp.arange(hot, dtype=jnp.int32)[:, None]).astype(jnp.int32), axis=1)


def cell_of(sorted_ids, owner, rank, shards, hot, capacity):
    return jnp.where(sorted_ids < hot, sorted_ids, jnp.minimum(hot + owner * capacity + rank, hot + shards * capacity - 1))


def exchange(rows, shards):
    return lax.all_to_all(rows.reshape(shards, -1, rows.shape[-1]), AXIS_NAME, 0, 0).reshape(rows.shape)


def exchange_ids(ids):
    return lax.all_to_all(ids, AXIS_NAME, 0, 0)


def dot(a, b, dims):
    return lax.dot_general(a, b, (dims, ((), ())), preferred_element_type=jnp.float32)


def after(value, earlier):
    return lax.optimization_barrier((value, earlier))


def when(predicate, update, value):
    return lax.while_loop(lambda state: state[0], lambda state: (jnp.zeros((), jnp.bool_), update(state[1])), (predicate, value))[1]


def plan_unique(sorted_ids, shard_rows, shards, capacity):
    previous = jnp.concatenate([jnp.full((1,), -1, jnp.int32), sorted_ids[:-1]])
    first = (sorted_ids != previous)
    owner = sorted_ids // shard_rows
    rank = running_count(first) - 1
    owners = jnp.arange(shards, dtype=jnp.int32)
    counts = jnp.sum((first[None, :] & (owner[None, :] == owners[:, None])).astype(jnp.int32), axis=1)
    starts = jnp.sum(jnp.where(owners[None, :] < owners[:, None], counts[None, :], 0), axis=1)
    start_of = jnp.sum(jnp.where(owner[:, None] == owners[None, :], starts[None, :], 0), axis=1)
    packed = lax.sort(jnp.where(first, sorted_ids, jnp.int32(NO_ID)))
    packed = jnp.concatenate([packed, jnp.full((capacity,), NO_ID, jnp.int32)])
    asked = jnp.stack([lax.dynamic_slice(packed, (starts[s],), (capacity,)) for s in range(shards)])
    return owner, rank - start_of, asked


def full_step(shards, in_shard, out_shard, center_ids, context_ids, negative_ids):
    shard_rows = in_shard.shape[0]
    num_pairs, num_negs = center_ids.shape[0], negative_ids.shape[0]
    cap_pairs, cap_negs = unique_capacity(num_pairs, shards), unique_capacity(num_negs, shards)
    me = lax.axis_index(AXIS_NAME)
    take = functools.partial(jnp.take, axis=0, mode='clip')
    neg_sorted = lax.sort(negative_ids)
    cen_sorted, con_moved = lax.sort((center_ids, context_ids), num_keys=1)
    con_sorted, con_pos = lax.sort((con_moved, jnp.arange(num_pairs, dtype=jnp.int32)), num_keys=1)

    def fetch(table, sorted_ids, capacity):
        owner, rank, asked = plan_unique(sorted_ids, shard_rows, shards, capacity)
        local = jnp.clip(exchange_ids(asked) - me * shard_rows, 0, shard_rows - 1).reshape(-1)
        return owner * capacity + rank, local, exchange(take(table, local), shards)

    neg_cell, neg_local, neg_got = fetch(out_shard, neg_sorted, cap_negs)
    cen_cell, cen_local, cen_got = fetch(in_shard, cen_sorted, cap_pairs)
    con_cell, con_local, con_got = fetch(out_shard, con_sorted, cap_pairs)
    con_cell = lax.sort((con_pos, con_cell), num_keys=1)[1]
    negative_half = split_rows([take(neg_got, neg_cell)], jnp.ones((num_negs,), jnp.float32))[0]
    center_vec = take(cen_got, cen_cell)
    center_half = split_rows([center_vec], jnp.ones((num_pairs,), jnp.float32))[0]
    neg_grad = (NEG_WEIGHT / num_negs * jax.nn.sigmoid(dot(center_half, negative_half, ((1,), (1,))))).astype(jnp.bfloat16)
    context_vec = take(con_got, con_cell)
    pos_grad = (jax.nn.sigmoid(jnp.sum(center_vec * context_vec, axis=1)) - 1.0)[:, None]
    d_center = dot(neg_grad, negative_half, ((1,), (0,))) + pos_grad * context_vec
    d_negative = dot(neg_grad, center_half, ((0,), (0,)))

    def give(table, grads, cell, local, capacity):
        sums = jax.ops.segment_sum(grads, cell, num_segments=shards * capacity)
        return table.at[local].add(-LEARN_RATE * exchange(sums, shards))

    new_out = give(out_shard, d_negative, neg_cell, neg_local, cap_negs)
    new_out = give(new_out, pos_grad * center_vec, con_cell, con_local, cap_pairs)
    return give(in_shard, d_center, cen_cell, cen_local, cap_pairs), new_out


def tight_step(shards, in_shard, out_shard, center_ids, context_ids, negative_ids):
    shard_rows = in_shard.shape[0]
    num_pairs, num_negs = center_ids.shape[0], negative_ids.shape[0]
    hot = HOT_ROWS
    cap_pairs, cap_negs = tight_capacity(num_pairs, shards), tight_capacity(num_negs, shards)
    me = lax.axis_index(AXIS_NAME)

    hot_both = jnp.concatenate([in_shard[:hot], out_shard[:hot]])
    hot_both = lax.psum(jnp.where(me == 0, hot_both, 0.0), AXIS_NAME)
    hot_in, hot_out = hot_both[:hot], hot_both[hot:]

    neg_sorted = lax.sort(negative_ids)
    neg_first, neg_owner, neg_rank, neg_counts = mark_unique(neg_sorted, shard_rows, shards, hot)
    neg_asked, neg_times = ask_lists(neg_sorted, neg_first, neg_owner, neg_rank, neg_counts, shard_rows, shards, cap_negs)

    cen_sorted, con_moved = lax.sort((center_ids, context_ids), num_keys=1)
    cen_first, cen_owner, cen_rank, cen_counts = mark_unique(cen_sorted, shard_rows, shards, hot)
    cen_asked, cen_times = ask_lists(cen_sorted, cen_first, cen_owner, cen_rank, cen_counts, shard_rows, shards, cap_pairs)
    cen_cell = cell_of(cen_sorted, cen_owner, cen_rank, shards, hot, cap_pairs)
    con_sorted, cen_by_con = lax.sort((con_moved, cen_cell), num_keys=1)
    con_first, con_owner, con_rank, con_counts = mark_unique(con_sorted, shard_rows, shards, hot)
    con_asked, _ = ask_lists(con_sorted, con_first, con_owner, con_rank, con_counts, shard_rows, shards, cap_pairs)
    con_cell = cell_of(con_sorted, con_owner, con_rank, shards, hot, cap_pairs)
    fits = (jnp.max(neg_counts) <= cap_negs) & (jnp.max(cen_counts) <= cap_pairs) & (jnp.max(con_counts) <= cap_pairs)
    spill = jnp.broadcast_to(1 - fits.astype(jnp.int32), (shards, 1))
    asked = exchange_ids(jnp.concatenate([cen_asked, con_asked, neg_asked, spill], axis=1))
    all_fit = jnp.sum(asked[:, -1]) == 0
    cen_local = asked[:, :cap_pairs] - me * shard_rows
    con_local = asked[:, cap_pairs:2 * cap_pairs] - me * shard_rows
    neg_local = asked[:, 2 * cap_pairs:-1] - me * shard_rows
    neg_send = gather_rows(out_shard, jnp.minimum(neg_local, shard_rows - 1).reshape(-1), shards)
    neg_got = exchange(neg_send, shards)
    cen_order, con_by_cen = lax.sort((cen_by_con, con_cell), num_keys=1)

    cen_send = gather_rows(in_shard, jnp.minimum(cen_local, shard_rows - 1).reshape(-1), shards)
    cen_send, neg_got, hot_in, hot_out = lax.optimization_barrier((cen_send, neg_got, hot_in, hot_out))
    cen_got = exchange(cen_send, shards)
    con_send = gather_rows(out_shard, jnp.minimum(con_local, shard_rows - 1).reshape(-1), shards)
    con_send, cen_got = after(con_send, cen_got)
    con_got = exchange(con_send, shards)

    neg_times = jnp.concatenate([hot_times(negative_ids, hot), neg_times])
    hot_cen_times = hot_times(center_ids, hot)
    w_half, w_high, w_low = split_rows([hot_out, neg_got], neg_times)
    uh_half, uh_high, uh_low = split_rows([hot_in], hot_cen_times)
    uc_half, uc_high, uc_low = split_rows([cen_got], cen_times)

    def neg_grads(u_half):
        return (NEG_WEIGHT / num_negs * jax.nn.sigmoid(dot(u_half, w_half, ((1,), (1,))))).astype(jnp.bfloat16)

    grad_h, grad_c = neg_grads(uh_half), neg_grads(uc_half)
    rows_in, cols_in = ((0,), (0,)), ((1,), (0,))

    def rest(times, half, high, low):
        return (times.astype(jnp.float32)[:, None] * half.astype(jnp.float32) - high.astype(jnp.float32) - low.astype(jnp.float32)).astype(jnp.bfloat16)

    d_neg = dot(grad_h, uh_high, rows_in) + dot(grad_h, uh_low, rows_in) + dot(grad_c, uc_high, rows_in)
    more = (jnp.max(cen_times) > 2) | (jnp.max(hot_cen_times) > 256)
    d_neg = when(more, lambda d: d + dot(grad_c, uc_low, rows_in) + dot(grad_h, rest(hot_cen_times, uh_half, uh_high, uh_low), rows_in) + dot(grad_c, rest(cen_times, uc_half, uc_high, uc_low), rows_in), d_neg)
    d_neg = jnp.where(neg_times[:, None] > 0, neg_times.astype(jnp.float32)[:, None] * d_neg, 0.0)
    neg_part, neg_hot = d_neg[hot:], d_neg[:hot]

    con_hot, con_part = pair_sums(hot_in, cen_got, hot_out, con_got, cen_by_con, con_cell)
    cen_hot, cen_part = pair_sums(hot_out, con_got, hot_in, cen_got, con_by_cen, cen_order)

    def center_grads(grad, times, pair_part):
        d = dot(grad, w_high, cols_in) + dot(grad[:, :hot], w_low[:hot], cols_in)
        more = (jnp.max(neg_times[hot:]) > 2) | (jnp.max(neg_times) > 256)
        d = when(more, lambda d: d + dot(grad[:, hot:], w_low[hot:], cols_in) + dot(grad, rest(neg_times, w_half, w_high, w_low), cols_in), d)
        return jnp.where(times[:, None] > 0, times.astype(jnp.float32)[:, None] * d + pair_part, 0.0)

    cen_hot = center_grads(grad_h, hot_cen_times, cen_hot)
    cen_part = center_grads(grad_c, cen_times, cen_part)

    neg_part, con_got = after(neg_part, con_got)
    neg_back = exchange(neg_part, shards)
    con_part, neg_back = after(con_part, neg_back)
    con_back = exchange(con_part, shards)
    out_hot = lax.psum(con_hot + neg_hot, AXIS_NAME)
    cen_part, con_back, out_hot = lax.optimization_barrier((cen_part, con_back, out_hot))
    cen_back = exchange(cen_part, shards)
    out_hot = jnp.where(me == 0, out_hot, 0.0)
    in_hot = jnp.where(me == 0, lax.psum(cen_hot, AXIS_NAME), 0.0)
    new_out = subtract_rows(out_shard, out_hot, [(neg_local, neg_back), (con_local, con_back)])
    new_in = subtract_rows(in_shard, in_hot, [(cen_local, cen_back)])
    return new_in, new_out, all_fit


def solution(mesh):
    shards = mesh.shape[AXIS_NAME]

    def device_step(*args):
        new_in, new_out, all_fit = tight_step(shards, *args)
        return when(~all_fit, lambda _: full_step(shards, *args), (new_in, new_out))

    return jax.shard_map(device_step, mesh=mesh, in_specs=(P(AXIS_NAME, None), P(AXIS_NAME, None), P(AXIS_NAME), P(AXIS_NAME), P(AXIS_NAME)), out_specs=(P(AXIS_NAME, None), P(AXIS_NAME, None)), check_vma=False)
```

```python
import functools

import jax
import jax.numpy as jnp
from jax import lax
from jax.experimental import pallas as pl
from jax.experimental.pallas import tpu as pltpu
from jax.sharding import PartitionSpec as P


LEARN_RATE = 1.0
NEG_WEIGHT = 5.0
AXIS_NAME = 'vp'
HOT_ROWS = 768
LANES = 128
SUBLANES = 8
PAIR_TILES = 4
NO_ID = 2**30
VMEM_BYTES = 60 * 2**20
ANY = pl.BlockSpec(memory_space=pl.ANY)


def unique_capacity(num_ids, shards):
    common_slots = 3 * num_ids // shards
    return common_slots // 4 + (num_ids - common_slots + shards - 1) // shards


def context_capacity(num_ids, shards):
    share = tight_capacity(num_ids, shards) * 5 // 8
    return share + 64, tight_capacity(num_ids, shards) - share + 64


def tight_capacity(num_ids, shards):
    return (num_ids - 3 * num_ids // shards + shards - 1) // shards


def tile_view(rows):
    n, d = rows.shape
    return rows.reshape(n // SUBLANES, SUBLANES, d // LANES, LANES).transpose(0, 2, 1, 3).reshape(n * d // LANES, LANES)


def row_view(lines, d):
    n = lines.shape[0] * LANES // d
    return lines.reshape(n // SUBLANES, d // LANES, SUBLANES, LANES).transpose(0, 2, 1, 3).reshape(n, d)


def first_line(row, d):
    return (row // SUBLANES) * (SUBLANES * (d // LANES)) + row % SUBLANES


def gather_rows(table, rows, groups):
    n, d = rows.shape[0], table.shape[1]
    chunks, cap = d // LANES, n // groups
    view = tile_view(table)

    def body(line, t_ref, o_ref):
        group = pl.program_id(0)

        def step(t, carry):
            start = group * cap + t * SUBLANES
            got = [t_ref[pl.ds(line[start + j], chunks, stride=SUBLANES), :] for j in range(SUBLANES)]
            for j in range(SUBLANES):
                o_ref[pl.ds(t * SUBLANES * chunks + j, chunks, stride=SUBLANES), :] = got[j]
            return carry

        lax.fori_loop(0, cap // SUBLANES, step, 0, unroll=2)

    out = pl.pallas_call(
        body,
        grid_spec=pltpu.PrefetchScalarGridSpec(
            num_scalar_prefetch=1, grid=(groups,),
            in_specs=[pl.BlockSpec(view.shape, lambda s, i: (0, 0), pipeline_mode=pl.Buffered(1))],
            out_specs=pl.BlockSpec((cap * chunks, LANES), lambda s, i: (s, 0))),
        out_shape=jax.ShapeDtypeStruct((n * chunks, LANES), table.dtype),
        cost_estimate=pl.CostEstimate(flops=0, bytes_accessed=4 * d * (table.shape[0] + 3 * n), transcendentals=0),
        compiler_params=pltpu.CompilerParams(vmem_limit_bytes=VMEM_BYTES),
        name='gather_rows',
    )(first_line(rows, d), view)
    return row_view(out, d)


def pair_sums(x_parts, y_parts, x_row, y_row, count, from_y=False):
    d = x_parts[0].shape[1]
    chunks, per_step = d // LANES, PAIR_TILES * SUBLANES
    views = [tile_view(a) for a in x_parts + y_parts]
    num_x, num_y = len(x_parts), len(y_parts)
    sizes = [v.shape[0] for v in views]
    x_lines, y_lines = sum(sizes[:num_x]), sum(sizes[num_x:])
    y_size = y_lines + SUBLANES * chunks
    y_starts = [sum(sizes[num_x:num_x + k]) for k in range(num_y)]

    def body(*refs):
        number, x_line, y_line = refs[:3]
        ins = refs[3:3 + num_x + num_y]
        outs = refs[3 + num_x + num_y:3 + num_x + 2 * num_y]
        x_all, y_all, total, prod, sem = refs[3 + num_x + 2 * num_y:]
        copies = []
        for k, ref in enumerate(ins):
            start = sum(sizes[:k]) if k < num_x else y_starts[k - num_x]
            held = x_all if k < num_x else y_all
            copies.append(pltpu.make_async_copy(ref, held.at[pl.ds(start, sizes[k])], sem.at[k]))
            if from_y and k >= num_x:
                copies.append(pltpu.make_async_copy(ref, total.at[pl.ds(start, sizes[k])], sem.at[k + num_y]))
        for copy in copies:
            copy.start()

        def zero(t, carry):
            total[pl.ds(pl.multiple_of(t * 64, 64), 64), :] = jnp.zeros((64, LANES), jnp.float32)
            return carry

        if not from_y:
            lax.fori_loop(0, y_lines // 64, zero, 0)
        for copy in copies:
            copy.wait()

        def step(t, carry):
            run, last = carry
            kept, lines, grads = [], [], []
            for i in range(per_step):
                tile, j = i // SUBLANES, i % SUBLANES
                line = y_line[t * per_step + i]
                x = x_all[pl.ds(x_line[t * per_step + i], chunks, stride=SUBLANES), :]
                y = y_all[pl.ds(line, chunks, stride=SUBLANES), :]
                prod[pl.ds(tile * SUBLANES * chunks + j, chunks, stride=SUBLANES), :] = x * y
                kept.append(x)
                lines.append(line)
            for tile in range(PAIR_TILES):
                part = prod[pl.ds(tile * SUBLANES * chunks, SUBLANES), :]
                for k in range(1, chunks):
                    part = part + prod[pl.ds((tile * chunks + k) * SUBLANES, SUBLANES), :]
                score = jnp.broadcast_to(jnp.sum(part, axis=1, keepdims=True), (SUBLANES, LANES))
                grads.append(jax.nn.sigmoid(score) - 1.0)
            for i in range(per_step):
                tile, j = i // SUBLANES, i % SUBLANES
                same = (lines[i] == last).astype(jnp.float32)
                run = run * same + jnp.broadcast_to(grads[tile][j:j + 1, :], (chunks, LANES)) * kept[i]
                at = pl.ds(lines[i], chunks, stride=SUBLANES)
                total[at, :] = y_all[at, :] - LEARN_RATE * run if from_y else run
                last = lines[i]
            return run, last

        lax.fori_loop(0, pl.cdiv(number[0], per_step), step, (jnp.zeros((chunks, LANES), jnp.float32), jnp.int32(-1)))
        copies = [pltpu.make_async_copy(total.at[pl.ds(y_starts[k], sizes[num_x + k])], outs[k], sem.at[k]) for k in range(num_y)]
        for copy in copies:
            copy.start()
        for copy in copies:
            copy.wait()

    results = pl.pallas_call(
        body,
        grid_spec=pltpu.PrefetchScalarGridSpec(
            num_scalar_prefetch=3, grid=(1,), in_specs=[ANY] * (num_x + num_y), out_specs=[ANY] * num_y,
            scratch_shapes=[pltpu.VMEM((x_lines, LANES), jnp.float32), pltpu.VMEM((y_size, LANES), jnp.float32),
                            pltpu.VMEM((y_size, LANES), jnp.float32), pltpu.VMEM((per_step * chunks, LANES), jnp.float32),
                            pltpu.SemaphoreType.DMA((num_x + 2 * num_y,))]),
        out_shape=[jax.ShapeDtypeStruct((n, LANES), jnp.float32) for n in sizes[num_x:]],
        cost_estimate=pl.CostEstimate(flops=0, bytes_accessed=8 * 4 * d * x_row.shape[0], transcendentals=0),
        compiler_params=pltpu.CompilerParams(vmem_limit_bytes=VMEM_BYTES),
        name='pair_sums',
    )(count.astype(jnp.int32).reshape(1), first_line(x_row, d), first_line(y_row, d), *views)
    return [row_view(r, d) for r in results]


def subtract_rows(table, hot, parts):
    d = table.shape[1]
    chunks, batch = d // LANES, 16
    groups = parts[0][0].shape[0]
    caps = [rows.shape[1] for rows, _ in parts]
    view, hot_view = tile_view(table), tile_view(hot)
    lines = view.shape[0]
    count = len(parts)

    def body(*refs):
        line = refs[:count]
        t_hbm, h_ref = refs[count:count + 2]
        values = refs[count + 2:2 * count + 2]
        o_hbm, held, sem = refs[2 * count + 2:]
        group = pl.program_id(0)

        @pl.when(group == 0)
        def _():
            copy = pltpu.make_async_copy(t_hbm, held.at[pl.ds(0, lines)], sem)
            copy.start()
            copy.wait()

            def hot_step(t, carry):
                window = pl.ds(pl.multiple_of(t * 64, 64), 64)
                held[window, :] = held[window, :] - LEARN_RATE * h_ref[window, :]
                return carry

            lax.fori_loop(0, h_ref.shape[0] // 64, hot_step, 0)

        for p in range(count):
            def step(t, carry, p=p):
                at = [line[p][group * caps[p] + t * batch + j] for j in range(batch)]
                new = []
                for j in range(batch):
                    source = (t * (batch // SUBLANES) + j // SUBLANES) * SUBLANES * chunks + j % SUBLANES
                    value = values[p][pl.ds(source, chunks, stride=SUBLANES), :]
                    new.append(held[pl.ds(at[j], chunks, stride=SUBLANES), :] - LEARN_RATE * value)
                for j in range(batch):
                    held[pl.ds(at[j], chunks, stride=SUBLANES), :] = new[j]
                return carry

            lax.fori_loop(0, caps[p] // batch, step, 0)

        @pl.when(group == groups - 1)
        def _():
            copy = pltpu.make_async_copy(held.at[pl.ds(0, lines)], o_hbm, sem)
            copy.start()
            copy.wait()

    out = pl.pallas_call(
        body,
        grid_spec=pltpu.PrefetchScalarGridSpec(
            num_scalar_prefetch=count, grid=(groups,),
            in_specs=[ANY, pl.BlockSpec(hot_view.shape, lambda s, *i: (0, 0))] + [pl.BlockSpec((c * chunks, LANES), lambda s, *i: (s, 0)) for c in caps],
            out_specs=ANY,
            scratch_shapes=[pltpu.VMEM((lines + SUBLANES * chunks, LANES), jnp.float32), pltpu.SemaphoreType.DMA]),
        out_shape=jax.ShapeDtypeStruct((lines, LANES), jnp.float32),
        cost_estimate=pl.CostEstimate(flops=0, bytes_accessed=4 * d * (2 * table.shape[0] + 3 * groups * sum(caps)), transcendentals=0),
        compiler_params=pltpu.CompilerParams(vmem_limit_bytes=VMEM_BYTES),
        name='subtract_rows',
    )(*[first_line(rows.reshape(-1), d) for rows, _ in parts], view, hot_view, *[tile_view(values) for _, values in parts])
    return row_view(out, d)


def split_rows(sources, times, block=256):
    d = sources[0].shape[1]
    blocks = [a.shape[0] // block for a in sources]
    starts = [sum(blocks[:k]) for k in range(len(blocks))]
    total = sum(blocks) * block

    def body(*refs):
        ins, t_ref, (r_ref, h_ref, l_ref) = refs[:len(sources)], refs[len(sources)], refs[len(sources) + 1:]
        step = pl.program_id(0)
        for k, ref in enumerate(ins):
            @pl.when((step >= starts[k]) & (step < starts[k] + blocks[k]))
            def _(ref=ref):
                rounded = ref[...].astype(jnp.bfloat16)
                scaled = rounded.astype(jnp.float32) * t_ref[...]
                high = scaled.astype(jnp.bfloat16)
                r_ref[...] = rounded
                h_ref[...] = high
                l_ref[...] = (scaled - high.astype(jnp.float32)).astype(jnp.bfloat16)

    def pick(k):
        return lambda i: (jnp.clip(i - starts[k], 0, blocks[k] - 1), 0)

    spec = pl.BlockSpec((block, d), lambda i: (i, 0))
    return pl.pallas_call(
        body, grid=(sum(blocks),),
        in_specs=[pl.BlockSpec((block, d), pick(k)) for k in range(len(sources))] + [pl.BlockSpec((block, 1), lambda i: (i, 0))],
        out_specs=[spec] * 3, out_shape=[jax.ShapeDtypeStruct((total, d), jnp.bfloat16)] * 3,
        cost_estimate=pl.CostEstimate(flops=0, bytes_accessed=10 * d * total, transcendentals=0),
        name='split_rows',
    )(*sources, times.astype(jnp.float32)[:, None])


def running_count(flags):
    rows = flags.shape[0] // LANES
    grid = flags.reshape(rows, LANES).astype(jnp.bfloat16)
    upper = (jnp.arange(LANES)[:, None] <= jnp.arange(LANES)[None, :]).astype(jnp.bfloat16)
    inner = jnp.dot(grid, upper, preferred_element_type=jnp.float32)
    lower = (jnp.arange(rows)[:, None] > jnp.arange(rows)[None, :]).astype(jnp.bfloat16)
    outer = jnp.dot(lower, inner[:, -1:].astype(jnp.bfloat16), preferred_element_type=jnp.float32)
    return (inner + outer).astype(jnp.int32).reshape(-1)


def mark_unique(sorted_ids, shard_rows, shards, hot, limit=NO_ID):
    previous = jnp.concatenate([jnp.full((1,), -1, jnp.int32), sorted_ids[:-1]])
    first = (sorted_ids != previous) & (sorted_ids >= hot) & (sorted_ids < limit)
    owner = sorted_ids // shard_rows
    rank = running_count(first) - 1
    owners = jnp.arange(shards, dtype=jnp.int32)
    counts = jnp.sum((first[None, :] & (owner[None, :] == owners[:, None])).astype(jnp.int32), axis=1)
    starts = jnp.sum(jnp.where(owners[None, :] < owners[:, None], counts[None, :], 0), axis=1)
    start_of = jnp.sum(jnp.where(owner[None, :] == owners[:, None], starts[:, None], 0), axis=0)
    return first, owner, rank - start_of, counts


def fill_cells(counts, capacity, shards):
    owners = jnp.arange(shards, dtype=jnp.int32)[:, None]
    slot = jnp.arange(capacity, dtype=jnp.int32)[None, :]
    return jnp.where(slot >= counts[:, None], owners * capacity + slot, NO_ID).reshape(-1)


def spread(values, capacity):
    return jnp.broadcast_to(values[:, None], (values.shape[0], capacity)).reshape(-1)


def ask_lists(sorted_ids, first, owner, rank, counts, shard_rows, shards, capacity):
    num_ids = sorted_ids.shape[0]
    cells = shards * capacity
    pack = 2 * num_ids
    key = jnp.where(first & (rank < capacity), owner * capacity + rank, NO_ID)
    past = (jnp.arange(shards, dtype=jnp.int32) + 1) * shard_rows
    ends = jnp.sum((sorted_ids[None, :] < past[:, None]).astype(jnp.int32), axis=1)
    packed = lax.sort((
        jnp.concatenate([key, fill_cells(counts, capacity, shards)]),
        jnp.concatenate([sorted_ids * pack + jnp.arange(num_ids, dtype=jnp.int32), spread(past * pack + ends, capacity)])), num_keys=1)[1][:cells]
    places = packed % pack
    times = jnp.concatenate([places[1:], jnp.full((1,), num_ids, jnp.int32)]) - places
    return (packed // pack).reshape(shards, capacity), times


def hot_times(ids, hot):
    return jnp.sum((ids[None, :] == jnp.arange(hot, dtype=jnp.int32)[:, None]).astype(jnp.int32), axis=1)


def cell_of(sorted_ids, owner, rank, shards, hot, capacity):
    return jnp.where(sorted_ids < hot, sorted_ids, jnp.minimum(hot + owner * capacity + rank, hot + shards * capacity - 1))


def exchange(rows, shards):
    return lax.all_to_all(rows.reshape(shards, -1, rows.shape[-1]), AXIS_NAME, 0, 0).reshape(rows.shape)


def exchange_ids(ids):
    return lax.all_to_all(ids, AXIS_NAME, 0, 0)


def dot(a, b, dims):
    return lax.dot_general(a, b, (dims, ((), ())), preferred_element_type=jnp.float32)


def after(value, earlier):
    return lax.optimization_barrier((value, earlier))


def when(predicate, update, value):
    return lax.while_loop(lambda state: state[0], lambda state: (jnp.zeros((), jnp.bool_), update(state[1])), (predicate, value))[1]


def plan_unique(sorted_ids, shard_rows, shards, capacity):
    previous = jnp.concatenate([jnp.full((1,), -1, jnp.int32), sorted_ids[:-1]])
    first = (sorted_ids != previous)
    owner = sorted_ids // shard_rows
    rank = running_count(first) - 1
    owners = jnp.arange(shards, dtype=jnp.int32)
    counts = jnp.sum((first[None, :] & (owner[None, :] == owners[:, None])).astype(jnp.int32), axis=1)
    starts = jnp.sum(jnp.where(owners[None, :] < owners[:, None], counts[None, :], 0), axis=1)
    start_of = jnp.sum(jnp.where(owner[:, None] == owners[None, :], starts[None, :], 0), axis=1)
    packed = lax.sort(jnp.where(first, sorted_ids, jnp.int32(NO_ID)))
    packed = jnp.concatenate([packed, jnp.full((capacity,), NO_ID, jnp.int32)])
    asked = jnp.stack([lax.dynamic_slice(packed, (starts[s],), (capacity,)) for s in range(shards)])
    return owner, rank - start_of, asked


def full_step(shards, in_shard, out_shard, center_ids, context_ids, negative_ids):
    shard_rows = in_shard.shape[0]
    num_pairs, num_negs = center_ids.shape[0], negative_ids.shape[0]
    cap_pairs, cap_negs = unique_capacity(num_pairs, shards), unique_capacity(num_negs, shards)
    me = lax.axis_index(AXIS_NAME)
    take = functools.partial(jnp.take, axis=0, mode='clip')
    neg_sorted = lax.sort(negative_ids)
    cen_sorted, con_moved = lax.sort((center_ids, context_ids), num_keys=1)
    con_sorted, con_pos = lax.sort((con_moved, jnp.arange(num_pairs, dtype=jnp.int32)), num_keys=1)

    def fetch(table, sorted_ids, capacity):
        owner, rank, asked = plan_unique(sorted_ids, shard_rows, shards, capacity)
        local = jnp.clip(exchange_ids(asked) - me * shard_rows, 0, shard_rows - 1).reshape(-1)
        return owner * capacity + rank, local, exchange(take(table, local), shards)

    neg_cell, neg_local, neg_got = fetch(out_shard, neg_sorted, cap_negs)
    cen_cell, cen_local, cen_got = fetch(in_shard, cen_sorted, cap_pairs)
    con_cell, con_local, con_got = fetch(out_shard, con_sorted, cap_pairs)
    con_cell = lax.sort((con_pos, con_cell), num_keys=1)[1]
    negative_half = split_rows([take(neg_got, neg_cell)], jnp.ones((num_negs,), jnp.float32))[0]
    center_vec = take(cen_got, cen_cell)
    center_half = split_rows([center_vec], jnp.ones((num_pairs,), jnp.float32))[0]
    neg_grad = (NEG_WEIGHT / num_negs * jax.nn.sigmoid(dot(center_half, negative_half, ((1,), (1,))))).astype(jnp.bfloat16)
    context_vec = take(con_got, con_cell)
    pos_grad = (jax.nn.sigmoid(jnp.sum(center_vec * context_vec, axis=1)) - 1.0)[:, None]
    d_center = dot(neg_grad, negative_half, ((1,), (0,))) + pos_grad * context_vec
    d_negative = dot(neg_grad, center_half, ((0,), (0,)))

    def give(table, grads, cell, local, capacity):
        sums = jax.ops.segment_sum(grads, cell, num_segments=shards * capacity)
        return table.at[local].add(-LEARN_RATE * exchange(sums, shards))

    new_out = give(out_shard, d_negative, neg_cell, neg_local, cap_negs)
    new_out = give(new_out, pos_grad * center_vec, con_cell, con_local, cap_pairs)
    return give(in_shard, d_center, cen_cell, cen_local, cap_pairs), new_out


def tight_step(shards, in_shard, out_shard, center_ids, context_ids, negative_ids):
    shard_rows = in_shard.shape[0]
    num_pairs, num_negs = center_ids.shape[0], negative_ids.shape[0]
    hot = HOT_ROWS
    cap_pairs, cap_negs = tight_capacity(num_pairs, shards), tight_capacity(num_negs, shards)
    me = lax.axis_index(AXIS_NAME)

    hot_both = jnp.concatenate([in_shard[:hot], out_shard[:hot]])
    hot_both = lax.psum(jnp.where(me == 0, hot_both, 0.0), AXIS_NAME)
    hot_in, hot_out = hot_both[:hot], hot_both[hot:]

    neg_sorted = lax.sort(negative_ids)
    neg_first, neg_owner, neg_rank, neg_counts = mark_unique(neg_sorted, shard_rows, shards, hot)
    neg_asked, neg_times = ask_lists(neg_sorted, neg_first, neg_owner, neg_rank, neg_counts, shard_rows, shards, cap_negs)

    cen_sorted, con_moved = lax.sort((center_ids, context_ids), num_keys=1)
    cen_first, cen_owner, cen_rank, cen_counts = mark_unique(cen_sorted, shard_rows, shards, hot)
    cen_asked, cen_times = ask_lists(cen_sorted, cen_first, cen_owner, cen_rank, cen_counts, shard_rows, shards, cap_pairs)
    cen_cell = cell_of(cen_sorted, cen_owner, cen_rank, shards, hot, cap_pairs)
    cap_con, cap_ship = context_capacity(num_pairs, shards)
    past_all = shards * shard_rows
    sent = (cen_sorted < hot) & (con_moved >= hot)
    con_keys, cen_by_con = lax.sort((con_moved + jnp.where(sent, past_all, 0), cen_cell), num_keys=1)
    stays = con_keys < past_all
    num_stay = jnp.sum(stays.astype(jnp.int32))
    con_first, con_owner, con_rank, con_counts = mark_unique(con_keys, shard_rows, shards, hot, past_all)
    con_cell = jnp.where(stays, cell_of(con_keys, con_owner, con_rank, shards, hot, cap_con), hot + shards * cap_con)
    sent_center = cen_by_con
    cen_key = jnp.where(stays, cen_by_con, hot + shards * cap_pairs)
    cen_by_con = jnp.where(stays, cen_by_con, 0)
    owners = jnp.arange(shards, dtype=jnp.int32)
    past = (owners + 1) * shard_rows
    ship_owner = con_owner - shards
    ship_upto = jnp.sum((con_keys[None, :] < (past + past_all)[:, None]).astype(jnp.int32), axis=1)
    ship_from = jnp.concatenate([num_stay[None], ship_upto[:-1]])
    ship_counts = ship_upto - ship_from
    from_of = jnp.sum(jnp.where(ship_owner[None, :] == owners[:, None], ship_from[:, None], 0), axis=0)
    ship_rank = jnp.arange(num_pairs, dtype=jnp.int32) - from_of
    con_cells = shards * cap_con
    key = jnp.where(con_first & (con_rank < cap_con), con_owner * cap_con + con_rank, NO_ID)
    key = jnp.where(stays | (ship_rank >= cap_ship), key, con_cells + ship_owner * cap_ship + ship_rank)
    ship_fill = fill_cells(ship_counts, cap_ship, shards)
    pack = 2 * hot
    both = lax.sort((
        jnp.concatenate([key, fill_cells(con_counts, cap_con, shards), jnp.where(ship_fill < NO_ID, con_cells + ship_fill, NO_ID)]),
        jnp.concatenate([jnp.where(stays, con_keys, (con_keys - past_all) * pack + sent_center), spread(past, cap_con), spread(past * pack + hot, cap_ship)])), num_keys=1)[1]
    con_asked = both[:con_cells].reshape(shards, cap_con)
    shipped = both[con_cells:con_cells + shards * cap_ship].reshape(shards, cap_ship)
    fits = (jnp.max(neg_counts) <= cap_negs) & (jnp.max(cen_counts) <= cap_pairs) & (jnp.max(con_counts) <= cap_con) & (jnp.max(ship_counts) <= cap_ship)
    spill = jnp.broadcast_to(1 - fits.astype(jnp.int32), (shards, 1))
    asked = exchange_ids(jnp.concatenate([cen_asked, con_asked, neg_asked, shipped, spill], axis=1))
    all_fit = jnp.sum(asked[:, -1]) == 0
    cuts = [0, cap_pairs, cap_pairs + cap_con, cap_pairs + cap_con + cap_negs, asked.shape[1] - 1]
    cen_local, con_local, neg_local = [asked[:, cuts[k]:cuts[k + 1]] - me * shard_rows for k in range(3)]
    taken = asked[:, cuts[3]:cuts[4]].reshape(-1)
    neg_send = gather_rows(out_shard, jnp.minimum(neg_local, shard_rows - 1).reshape(-1), shards)
    neg_got = exchange(neg_send, shards)
    cen_order, con_by_cen = lax.sort((cen_key, jnp.where(stays, con_cell, 0)), num_keys=1)

    cen_send = gather_rows(in_shard, jnp.minimum(cen_local, shard_rows - 1).reshape(-1), shards)
    cen_send, neg_got, hot_in, hot_out = lax.optimization_barrier((cen_send, neg_got, hot_in, hot_out))
    cen_got = exchange(cen_send, shards)
    con_send = gather_rows(out_shard, jnp.minimum(con_local, shard_rows - 1).reshape(-1), shards)
    con_send, cen_got = after(con_send, cen_got)
    con_got = exchange(con_send, shards)

    taken_by_con = lax.sort(taken - me * shard_rows * pack)
    taken_by_cen = lax.sort((taken % pack) * (2 * shard_rows) + taken // pack - me * shard_rows)
    num_taken = jnp.sum((taken % pack < hot).astype(jnp.int32))
    base_out, = pair_sums([hot_in], [out_shard], jnp.minimum(taken_by_con % pack, hot - 1), taken_by_con // pack, num_taken, True)
    ship_hot, = pair_sums([out_shard], [hot_in], jnp.minimum(taken_by_cen % (2 * shard_rows), shard_rows - 1), taken_by_cen // (2 * shard_rows), num_taken)

    neg_times = jnp.concatenate([hot_times(negative_ids, hot), neg_times])
    hot_cen_times = hot_times(center_ids, hot)
    w_half, w_high, w_low = split_rows([hot_out, neg_got], neg_times)
    uh_half, uh_high, uh_low = split_rows([hot_in], hot_cen_times)
    uc_half, uc_high, uc_low = split_rows([cen_got], cen_times)

    def neg_grads(u_half):
        return (NEG_WEIGHT / num_negs * jax.nn.sigmoid(dot(u_half, w_half, ((1,), (1,))))).astype(jnp.bfloat16)

    grad_h, grad_c = neg_grads(uh_half), neg_grads(uc_half)
    rows_in, cols_in = ((0,), (0,)), ((1,), (0,))

    def rest(times, half, high, low):
        return (times.astype(jnp.float32)[:, None] * half.astype(jnp.float32) - high.astype(jnp.float32) - low.astype(jnp.float32)).astype(jnp.bfloat16)

    d_neg = dot(grad_h, uh_high, rows_in) + dot(grad_h, uh_low, rows_in) + dot(grad_c, uc_high, rows_in)
    more = (jnp.max(cen_times) > 2) | (jnp.max(hot_cen_times) > 256)
    d_neg = when(more, lambda d: d + dot(grad_c, uc_low, rows_in) + dot(grad_h, rest(hot_cen_times, uh_half, uh_high, uh_low), rows_in) + dot(grad_c, rest(cen_times, uc_half, uc_high, uc_low), rows_in), d_neg)
    d_neg = jnp.where(neg_times[:, None] > 0, neg_times.astype(jnp.float32)[:, None] * d_neg, 0.0)
    neg_part, neg_hot = d_neg[hot:], d_neg[:hot]

    con_hot, con_part = pair_sums([hot_in, cen_got], [hot_out, con_got], cen_by_con, con_cell, num_stay)
    cen_hot, cen_part = pair_sums([hot_out, con_got], [hot_in, cen_got], con_by_cen, cen_order, num_stay)

    def center_grads(grad, times, pair_part):
        d = dot(grad, w_high, cols_in) + dot(grad[:, :hot], w_low[:hot], cols_in)
        more = (jnp.max(neg_times[hot:]) > 2) | (jnp.max(neg_times) > 256)
        d = when(more, lambda d: d + dot(grad[:, hot:], w_low[hot:], cols_in) + dot(grad, rest(neg_times, w_half, w_high, w_low), cols_in), d)
        return jnp.where(times[:, None] > 0, times.astype(jnp.float32)[:, None] * d + pair_part, 0.0)

    cen_hot = center_grads(grad_h, hot_cen_times, cen_hot) + ship_hot
    cen_part = center_grads(grad_c, cen_times, cen_part)

    neg_part, con_got = after(neg_part, con_got)
    neg_back = exchange(neg_part, shards)
    con_part, neg_back = after(con_part, neg_back)
    con_back = exchange(con_part, shards)
    out_hot = lax.psum(con_hot + neg_hot, AXIS_NAME)
    cen_part, con_back, out_hot, cen_hot = lax.optimization_barrier((cen_part, con_back, out_hot, cen_hot))
    cen_back = exchange(cen_part, shards)
    out_hot = jnp.where(me == 0, out_hot, 0.0)
    in_hot = lax.psum(cen_hot, AXIS_NAME)
    in_hot = jnp.where(me == 0, in_hot, 0.0)
    new_out = subtract_rows(base_out, out_hot, [(neg_local, neg_back), (con_local, con_back)])
    new_in = subtract_rows(in_shard, in_hot, [(cen_local, cen_back)])
    return new_in, new_out, all_fit


def solution(mesh):
    shards = mesh.shape[AXIS_NAME]

    def device_step(*args):
        new_in, new_out, all_fit = tight_step(shards, *args)
        return when(~all_fit, lambda _: full_step(shards, *args), (new_in, new_out))

    return jax.shard_map(device_step, mesh=mesh, in_specs=(P(AXIS_NAME, None), P(AXIS_NAME, None), P(AXIS_NAME), P(AXIS_NAME), P(AXIS_NAME)), out_specs=(P(AXIS_NAME, None), P(AXIS_NAME, None)), check_vma=False)
```

```python
import functools

import jax
import jax.numpy as jnp
from jax import lax
from jax.experimental import pallas as pl
from jax.experimental.pallas import tpu as pltpu
from jax.sharding import PartitionSpec as P


LEARN_RATE = 1.0
NEG_WEIGHT = 5.0
AXIS_NAME = 'vp'
HOT_ROWS = 768
LANES = 128
SUBLANES = 8
PAIR_TILES = 4
NO_ID = 2**30
VMEM_BYTES = 60 * 2**20
ANY = pl.BlockSpec(memory_space=pl.ANY)


def unique_capacity(num_ids, shards):
    common_slots = 3 * num_ids // shards
    return common_slots // 4 + (num_ids - common_slots + shards - 1) // shards


def context_capacity(num_ids, shards):
    share = tight_capacity(num_ids, shards) * 5 // 8
    return share + 64, tight_capacity(num_ids, shards) - share + 64


def tight_capacity(num_ids, shards):
    return (num_ids - 3 * num_ids // shards + shards - 1) // shards


def tile_view(rows):
    n, d = rows.shape
    return rows.reshape(n // SUBLANES, SUBLANES, d // LANES, LANES).transpose(0, 2, 1, 3).reshape(n * d // LANES, LANES)


def row_view(lines, d):
    n = lines.shape[0] * LANES // d
    return lines.reshape(n // SUBLANES, d // LANES, SUBLANES, LANES).transpose(0, 2, 1, 3).reshape(n, d)


def first_line(row, d):
    return (row // SUBLANES) * (SUBLANES * (d // LANES)) + row % SUBLANES


def gather_rows(table, rows, groups):
    n, d = rows.shape[0], table.shape[1]
    chunks, cap = d // LANES, n // groups
    view = tile_view(table)

    def body(line, t_ref, o_ref):
        group = pl.program_id(0)

        def step(t, carry):
            start = group * cap + t * SUBLANES
            got = [t_ref[pl.ds(line[start + j], chunks, stride=SUBLANES), :] for j in range(SUBLANES)]
            for j in range(SUBLANES):
                o_ref[pl.ds(t * SUBLANES * chunks + j, chunks, stride=SUBLANES), :] = got[j]
            return carry

        lax.fori_loop(0, cap // SUBLANES, step, 0, unroll=2)

    out = pl.pallas_call(
        body,
        grid_spec=pltpu.PrefetchScalarGridSpec(
            num_scalar_prefetch=1, grid=(groups,),
            in_specs=[pl.BlockSpec(view.shape, lambda s, i: (0, 0), pipeline_mode=pl.Buffered(1))],
            out_specs=pl.BlockSpec((cap * chunks, LANES), lambda s, i: (s, 0))),
        out_shape=jax.ShapeDtypeStruct((n * chunks, LANES), table.dtype),
        cost_estimate=pl.CostEstimate(flops=0, bytes_accessed=4 * d * (table.shape[0] + 3 * n), transcendentals=0),
        compiler_params=pltpu.CompilerParams(vmem_limit_bytes=VMEM_BYTES),
        name='gather_rows',
    )(first_line(rows, d), view)
    return row_view(out, d)


def pair_sums(x_parts, y_parts, x_row, y_row, count, from_y=False):
    d = x_parts[0].shape[1]
    chunks, per_step = d // LANES, PAIR_TILES * SUBLANES
    views = [tile_view(a) for a in x_parts + y_parts]
    num_x, num_y = len(x_parts), len(y_parts)
    sizes = [v.shape[0] for v in views]
    x_lines, y_lines = sum(sizes[:num_x]), sum(sizes[num_x:])
    y_size = y_lines + SUBLANES * chunks
    y_starts = [sum(sizes[num_x:num_x + k]) for k in range(num_y)]

    def body(*refs):
        number, x_line, y_line = refs[:3]
        ins = refs[3:3 + num_x + num_y]
        outs = refs[3 + num_x + num_y:3 + num_x + 2 * num_y]
        x_all, y_all, total, prod, sem = refs[3 + num_x + 2 * num_y:]
        copies = []
        for k, ref in enumerate(ins):
            start = sum(sizes[:k]) if k < num_x else y_starts[k - num_x]
            held = x_all if k < num_x else y_all
            copies.append(pltpu.make_async_copy(ref, held.at[pl.ds(start, sizes[k])], sem.at[k]))
            if from_y and k >= num_x:
                copies.append(pltpu.make_async_copy(ref, total.at[pl.ds(start, sizes[k])], sem.at[k + num_y]))
        for copy in copies:
            copy.start()

        def zero(t, carry):
            total[pl.ds(pl.multiple_of(t * 64, 64), 64), :] = jnp.zeros((64, LANES), jnp.float32)
            return carry

        if not from_y:
            lax.fori_loop(0, y_lines // 64, zero, 0)
        for copy in copies:
            copy.wait()

        def step(t, carry):
            run, last = carry
            kept, lines, grads = [], [], []
            for i in range(per_step):
                tile, j = i // SUBLANES, i % SUBLANES
                line = y_line[t * per_step + i]
                x = x_all[pl.ds(x_line[t * per_step + i], chunks, stride=SUBLANES), :]
                y = y_all[pl.ds(line, chunks, stride=SUBLANES), :]
                prod[pl.ds(tile * SUBLANES * chunks + j, chunks, stride=SUBLANES), :] = x * y
                kept.append(x)
                lines.append(line)
            for tile in range(PAIR_TILES):
                part = prod[pl.ds(tile * SUBLANES * chunks, SUBLANES), :]
                for k in range(1, chunks):
                    part = part + prod[pl.ds((tile * chunks + k) * SUBLANES, SUBLANES), :]
                score = jnp.broadcast_to(jnp.sum(part, axis=1, keepdims=True), (SUBLANES, LANES))
                grads.append(jax.nn.sigmoid(score) - 1.0)
            for i in range(per_step):
                tile, j = i // SUBLANES, i % SUBLANES
                same = (lines[i] == last).astype(jnp.float32)
                run = run * same + jnp.broadcast_to(grads[tile][j:j + 1, :], (chunks, LANES)) * kept[i]
                at = pl.ds(lines[i], chunks, stride=SUBLANES)
                total[at, :] = y_all[at, :] - LEARN_RATE * run if from_y else run
                last = lines[i]
            return run, last

        lax.fori_loop(0, pl.cdiv(number[0], per_step), step, (jnp.zeros((chunks, LANES), jnp.float32), jnp.int32(-1)))
        copies = [pltpu.make_async_copy(total.at[pl.ds(y_starts[k], sizes[num_x + k])], outs[k], sem.at[k]) for k in range(num_y)]
        for copy in copies:
            copy.start()
        for copy in copies:
            copy.wait()

    results = pl.pallas_call(
        body,
        grid_spec=pltpu.PrefetchScalarGridSpec(
            num_scalar_prefetch=3, grid=(1,), in_specs=[ANY] * (num_x + num_y), out_specs=[ANY] * num_y,
            scratch_shapes=[pltpu.VMEM((x_lines, LANES), jnp.float32), pltpu.VMEM((y_size, LANES), jnp.float32),
                            pltpu.VMEM((y_size, LANES), jnp.float32), pltpu.VMEM((per_step * chunks, LANES), jnp.float32),
                            pltpu.SemaphoreType.DMA((num_x + 2 * num_y,))]),
        out_shape=[jax.ShapeDtypeStruct((n, LANES), jnp.float32) for n in sizes[num_x:]],
        cost_estimate=pl.CostEstimate(flops=0, bytes_accessed=8 * 4 * d * x_row.shape[0], transcendentals=0),
        compiler_params=pltpu.CompilerParams(vmem_limit_bytes=VMEM_BYTES),
        name='pair_sums',
    )(count.astype(jnp.int32).reshape(1), first_line(x_row, d), first_line(y_row, d), *views)
    return [row_view(r, d) for r in results]


def subtract_rows(table, hot, parts):
    d = table.shape[1]
    chunks, batch = d // LANES, 16
    groups = parts[0][0].shape[0]
    caps = [rows.shape[1] for rows, _ in parts]
    view, hot_view = tile_view(table), tile_view(hot)
    lines = view.shape[0]
    count = len(parts)

    def body(*refs):
        line = refs[:count]
        t_hbm, h_ref = refs[count:count + 2]
        values = refs[count + 2:2 * count + 2]
        o_hbm, held, sem = refs[2 * count + 2:]
        group = pl.program_id(0)

        @pl.when(group == 0)
        def _():
            copy = pltpu.make_async_copy(t_hbm, held.at[pl.ds(0, lines)], sem)
            copy.start()
            copy.wait()

            def hot_step(t, carry):
                window = pl.ds(pl.multiple_of(t * 64, 64), 64)
                held[window, :] = held[window, :] - LEARN_RATE * h_ref[window, :]
                return carry

            lax.fori_loop(0, h_ref.shape[0] // 64, hot_step, 0)

        for p in range(count):
            def step(t, carry, p=p):
                at = [line[p][group * caps[p] + t * batch + j] for j in range(batch)]
                new = []
                for j in range(batch):
                    source = (t * (batch // SUBLANES) + j // SUBLANES) * SUBLANES * chunks + j % SUBLANES
                    value = values[p][pl.ds(source, chunks, stride=SUBLANES), :]
                    new.append(held[pl.ds(at[j], chunks, stride=SUBLANES), :] - LEARN_RATE * value)
                for j in range(batch):
                    held[pl.ds(at[j], chunks, stride=SUBLANES), :] = new[j]
                return carry

            lax.fori_loop(0, caps[p] // batch, step, 0)

        @pl.when(group == groups - 1)
        def _():
            copy = pltpu.make_async_copy(held.at[pl.ds(0, lines)], o_hbm, sem)
            copy.start()
            copy.wait()

    out = pl.pallas_call(
        body,
        grid_spec=pltpu.PrefetchScalarGridSpec(
            num_scalar_prefetch=count, grid=(groups,),
            in_specs=[ANY, pl.BlockSpec(hot_view.shape, lambda s, *i: (0, 0))] + [pl.BlockSpec((c * chunks, LANES), lambda s, *i: (s, 0)) for c in caps],
            out_specs=ANY,
            scratch_shapes=[pltpu.VMEM((lines + SUBLANES * chunks, LANES), jnp.float32), pltpu.SemaphoreType.DMA]),
        out_shape=jax.ShapeDtypeStruct((lines, LANES), jnp.float32),
        cost_estimate=pl.CostEstimate(flops=0, bytes_accessed=4 * d * (2 * table.shape[0] + 3 * groups * sum(caps)), transcendentals=0),
        compiler_params=pltpu.CompilerParams(vmem_limit_bytes=VMEM_BYTES),
        name='subtract_rows',
    )(*[first_line(rows.reshape(-1), d) for rows, _ in parts], view, hot_view, *[tile_view(values) for _, values in parts])
    return row_view(out, d)


def split_rows(sources, times, block=256):
    d = sources[0].shape[1]
    blocks = [a.shape[0] // block for a in sources]
    starts = [sum(blocks[:k]) for k in range(len(blocks))]
    total = sum(blocks) * block

    def body(*refs):
        ins, t_ref, (r_ref, h_ref, l_ref) = refs[:len(sources)], refs[len(sources)], refs[len(sources) + 1:]
        step = pl.program_id(0)
        for k, ref in enumerate(ins):
            @pl.when((step >= starts[k]) & (step < starts[k] + blocks[k]))
            def _(ref=ref):
                rounded = ref[...].astype(jnp.bfloat16)
                scaled = rounded.astype(jnp.float32) * t_ref[...]
                high = scaled.astype(jnp.bfloat16)
                r_ref[...] = rounded
                h_ref[...] = high
                l_ref[...] = (scaled - high.astype(jnp.float32)).astype(jnp.bfloat16)

    def pick(k):
        return lambda i: (jnp.clip(i - starts[k], 0, blocks[k] - 1), 0)

    spec = pl.BlockSpec((block, d), lambda i: (i, 0))
    return pl.pallas_call(
        body, grid=(sum(blocks),),
        in_specs=[pl.BlockSpec((block, d), pick(k)) for k in range(len(sources))] + [pl.BlockSpec((block, 1), lambda i: (i, 0))],
        out_specs=[spec] * 3, out_shape=[jax.ShapeDtypeStruct((total, d), jnp.bfloat16)] * 3,
        cost_estimate=pl.CostEstimate(flops=0, bytes_accessed=10 * d * total, transcendentals=0),
        name='split_rows',
    )(*sources, times.astype(jnp.float32)[:, None])


def running_count(flags):
    rows = flags.shape[0] // LANES
    grid = flags.reshape(rows, LANES).astype(jnp.bfloat16)
    upper = (jnp.arange(LANES)[:, None] <= jnp.arange(LANES)[None, :]).astype(jnp.bfloat16)
    inner = jnp.dot(grid, upper, preferred_element_type=jnp.float32)
    lower = (jnp.arange(rows)[:, None] > jnp.arange(rows)[None, :]).astype(jnp.bfloat16)
    outer = jnp.dot(lower, inner[:, -1:].astype(jnp.bfloat16), preferred_element_type=jnp.float32)
    return (inner + outer).astype(jnp.int32).reshape(-1)


def mark_unique(sorted_ids, shard_rows, shards, hot, limit=NO_ID):
    previous = jnp.concatenate([jnp.full((1,), -1, jnp.int32), sorted_ids[:-1]])
    first = (sorted_ids != previous) & (sorted_ids >= hot) & (sorted_ids < limit)
    owner = sorted_ids // shard_rows
    rank = running_count(first) - 1
    owners = jnp.arange(shards, dtype=jnp.int32)
    counts = jnp.sum((first[None, :] & (owner[None, :] == owners[:, None])).astype(jnp.int32), axis=1)
    starts = jnp.sum(jnp.where(owners[None, :] < owners[:, None], counts[None, :], 0), axis=1)
    start_of = jnp.sum(jnp.where(owner[None, :] == owners[:, None], starts[:, None], 0), axis=0)
    return first, owner, rank - start_of, counts


def fill_cells(counts, capacity, shards):
    owners = jnp.arange(shards, dtype=jnp.int32)[:, None]
    slot = jnp.arange(capacity, dtype=jnp.int32)[None, :]
    return jnp.where(slot >= counts[:, None], owners * capacity + slot, NO_ID).reshape(-1)


def spread(values, capacity):
    return jnp.broadcast_to(values[:, None], (values.shape[0], capacity)).reshape(-1)


def ask_lists(sorted_ids, first, owner, rank, counts, shard_rows, shards, capacity):
    num_ids = sorted_ids.shape[0]
    cells = shards * capacity
    pack = 2 * num_ids
    key = jnp.where(first & (rank < capacity), owner * capacity + rank, NO_ID)
    past = (jnp.arange(shards, dtype=jnp.int32) + 1) * shard_rows
    ends = jnp.sum((sorted_ids[None, :] < past[:, None]).astype(jnp.int32), axis=1)
    packed = lax.sort((
        jnp.concatenate([key, fill_cells(counts, capacity, shards)]),
        jnp.concatenate([sorted_ids * pack + jnp.arange(num_ids, dtype=jnp.int32), spread(past * pack + ends, capacity)])), num_keys=1)[1][:cells]
    places = packed % pack
    times = jnp.concatenate([places[1:], jnp.full((1,), num_ids, jnp.int32)]) - places
    return (packed // pack).reshape(shards, capacity), times


def hot_times(ids, hot):
    return jnp.sum((ids[None, :] == jnp.arange(hot, dtype=jnp.int32)[:, None]).astype(jnp.int32), axis=1)


def cell_of(sorted_ids, owner, rank, shards, hot, capacity):
    return jnp.where(sorted_ids < hot, sorted_ids, jnp.minimum(hot + owner * capacity + rank, hot + shards * capacity - 1))


def exchange(rows, shards):
    return lax.all_to_all(rows.reshape(shards, -1, rows.shape[-1]), AXIS_NAME, 0, 0).reshape(rows.shape)


def exchange_ids(ids):
    return lax.all_to_all(ids, AXIS_NAME, 0, 0)


def dot(a, b, dims):
    return lax.dot_general(a, b, (dims, ((), ())), preferred_element_type=jnp.float32)


def after(value, earlier):
    return lax.optimization_barrier((value, earlier))


def when(predicate, update, value):
    return lax.while_loop(lambda state: state[0], lambda state: (jnp.zeros((), jnp.bool_), update(state[1])), (predicate, value))[1]


def plan_unique(sorted_ids, shard_rows, shards, capacity):
    previous = jnp.concatenate([jnp.full((1,), -1, jnp.int32), sorted_ids[:-1]])
    first = (sorted_ids != previous)
    owner = sorted_ids // shard_rows
    rank = running_count(first) - 1
    owners = jnp.arange(shards, dtype=jnp.int32)
    counts = jnp.sum((first[None, :] & (owner[None, :] == owners[:, None])).astype(jnp.int32), axis=1)
    starts = jnp.sum(jnp.where(owners[None, :] < owners[:, None], counts[None, :], 0), axis=1)
    start_of = jnp.sum(jnp.where(owner[:, None] == owners[None, :], starts[None, :], 0), axis=1)
    packed = lax.sort(jnp.where(first, sorted_ids, jnp.int32(NO_ID)))
    packed = jnp.concatenate([packed, jnp.full((capacity,), NO_ID, jnp.int32)])
    asked = jnp.stack([lax.dynamic_slice(packed, (starts[s],), (capacity,)) for s in range(shards)])
    return owner, rank - start_of, asked


def full_step(shards, in_shard, out_shard, center_ids, context_ids, negative_ids):
    shard_rows = in_shard.shape[0]
    num_pairs, num_negs = center_ids.shape[0], negative_ids.shape[0]
    cap_pairs, cap_negs = unique_capacity(num_pairs, shards), unique_capacity(num_negs, shards)
    me = lax.axis_index(AXIS_NAME)
    take = functools.partial(jnp.take, axis=0, mode='clip')
    neg_sorted = lax.sort(negative_ids)
    cen_sorted, con_moved = lax.sort((center_ids, context_ids), num_keys=1)
    con_sorted, con_pos = lax.sort((con_moved, jnp.arange(num_pairs, dtype=jnp.int32)), num_keys=1)

    def fetch(table, sorted_ids, capacity):
        owner, rank, asked = plan_unique(sorted_ids, shard_rows, shards, capacity)
        local = jnp.clip(exchange_ids(asked) - me * shard_rows, 0, shard_rows - 1).reshape(-1)
        return owner * capacity + rank, local, exchange(take(table, local), shards)

    neg_cell, neg_local, neg_got = fetch(out_shard, neg_sorted, cap_negs)
    cen_cell, cen_local, cen_got = fetch(in_shard, cen_sorted, cap_pairs)
    con_cell, con_local, con_got = fetch(out_shard, con_sorted, cap_pairs)
    con_cell = lax.sort((con_pos, con_cell), num_keys=1)[1]
    negative_half = split_rows([take(neg_got, neg_cell)], jnp.ones((num_negs,), jnp.float32))[0]
    center_vec = take(cen_got, cen_cell)
    center_half = split_rows([center_vec], jnp.ones((num_pairs,), jnp.float32))[0]
    neg_grad = (NEG_WEIGHT / num_negs * jax.nn.sigmoid(dot(center_half, negative_half, ((1,), (1,))))).astype(jnp.bfloat16)
    context_vec = take(con_got, con_cell)
    pos_grad = (jax.nn.sigmoid(jnp.sum(center_vec * context_vec, axis=1)) - 1.0)[:, None]
    d_center = dot(neg_grad, negative_half, ((1,), (0,))) + pos_grad * context_vec
    d_negative = dot(neg_grad, center_half, ((0,), (0,)))

    def give(table, grads, cell, local, capacity):
        sums = jax.ops.segment_sum(grads, cell, num_segments=shards * capacity)
        return table.at[local].add(-LEARN_RATE * exchange(sums, shards))

    new_out = give(out_shard, d_negative, neg_cell, neg_local, cap_negs)
    new_out = give(new_out, pos_grad * center_vec, con_cell, con_local, cap_pairs)
    return give(in_shard, d_center, cen_cell, cen_local, cap_pairs), new_out


def tight_step(shards, in_shard, out_shard, center_ids, context_ids, negative_ids):
    shard_rows = in_shard.shape[0]
    num_pairs, num_negs = center_ids.shape[0], negative_ids.shape[0]
    hot = HOT_ROWS
    cap_pairs, cap_negs = tight_capacity(num_pairs, shards), tight_capacity(num_negs, shards)
    me = lax.axis_index(AXIS_NAME)

    hot_both = jnp.concatenate([in_shard[:hot], out_shard[:hot]])
    hot_both = lax.psum(jnp.where(me == 0, hot_both, 0.0), AXIS_NAME)
    hot_in, hot_out = hot_both[:hot], hot_both[hot:]

    neg_sorted = lax.sort(negative_ids)
    neg_first, neg_owner, neg_rank, neg_counts = mark_unique(neg_sorted, shard_rows, shards, hot)
    neg_asked, neg_times = ask_lists(neg_sorted, neg_first, neg_owner, neg_rank, neg_counts, shard_rows, shards, cap_negs)

    cen_sorted, con_moved = lax.sort((center_ids, context_ids), num_keys=1)
    cen_first, cen_owner, cen_rank, cen_counts = mark_unique(cen_sorted, shard_rows, shards, hot)
    cen_asked, cen_times = ask_lists(cen_sorted, cen_first, cen_owner, cen_rank, cen_counts, shard_rows, shards, cap_pairs)
    cen_cell = cell_of(cen_sorted, cen_owner, cen_rank, shards, hot, cap_pairs)
    cap_con, cap_ship = context_capacity(num_pairs, shards)
    past_all = shards * shard_rows
    sent = (cen_sorted < hot) & (con_moved >= hot)
    con_keys, cen_by_con = lax.sort((con_moved + jnp.where(sent, past_all, 0), cen_cell), num_keys=1)
    stays = con_keys < past_all
    num_stay = jnp.sum(stays.astype(jnp.int32))
    con_first, con_owner, con_rank, con_counts = mark_unique(con_keys, shard_rows, shards, hot, past_all)
    con_cell = jnp.where(stays, cell_of(con_keys, con_owner, con_rank, shards, hot, cap_con), hot + shards * cap_con)
    sent_center = cen_by_con
    cen_key = jnp.where(stays, cen_by_con, hot + shards * cap_pairs)
    cen_by_con = jnp.where(stays, cen_by_con, 0)
    owners = jnp.arange(shards, dtype=jnp.int32)
    past = (owners + 1) * shard_rows
    ship_owner = con_owner - shards
    ship_upto = jnp.sum((con_keys[None, :] < (past + past_all)[:, None]).astype(jnp.int32), axis=1)
    ship_from = jnp.sum((con_keys[None, :] < (past - shard_rows + past_all)[:, None]).astype(jnp.int32), axis=1)
    ship_counts = ship_upto - ship_from
    from_of = jnp.sum(jnp.where(ship_owner[None, :] == owners[:, None], ship_from[:, None], 0), axis=0)
    ship_rank = jnp.arange(num_pairs, dtype=jnp.int32) - from_of
    con_cells = shards * cap_con
    key = jnp.where(con_first & (con_rank < cap_con), con_owner * cap_con + con_rank, NO_ID)
    key = jnp.where(stays | (ship_rank >= cap_ship), key, con_cells + ship_owner * cap_ship + ship_rank)
    ship_fill = fill_cells(ship_counts, cap_ship, shards)
    pack = 2 * hot
    both = lax.sort((
        jnp.concatenate([key, fill_cells(con_counts, cap_con, shards), jnp.where(ship_fill < NO_ID, con_cells + ship_fill, NO_ID)]),
        jnp.concatenate([jnp.where(stays, con_keys, (con_keys - past_all) * pack + sent_center), spread(past, cap_con), spread(past * pack + hot, cap_ship)])), num_keys=1)[1]
    con_asked = both[:con_cells].reshape(shards, cap_con)
    shipped = both[con_cells:con_cells + shards * cap_ship].reshape(shards, cap_ship)
    over = (neg_counts > cap_negs) | (cen_counts > cap_pairs) | (con_counts > cap_con) | (ship_counts > cap_ship)
    spill = jnp.broadcast_to(over.astype(jnp.int32)[None, :], (shards, shards))
    asked = exchange_ids(jnp.concatenate([cen_asked, con_asked, neg_asked, shipped, spill], axis=1))
    all_fit = jnp.sum(asked[:, -shards:]) == 0
    cuts = [0, cap_pairs, cap_pairs + cap_con, cap_pairs + cap_con + cap_negs, asked.shape[1] - shards]
    cen_local, con_local, neg_local = [asked[:, cuts[k]:cuts[k + 1]] - me * shard_rows for k in range(3)]
    taken = asked[:, cuts[3]:cuts[4]].reshape(-1)
    neg_send = gather_rows(out_shard, jnp.minimum(neg_local, shard_rows - 1).reshape(-1), shards)
    neg_got = exchange(neg_send, shards)
    cen_order, con_by_cen = lax.sort((cen_key, jnp.where(stays, con_cell, 0)), num_keys=1)

    cen_send = gather_rows(in_shard, jnp.minimum(cen_local, shard_rows - 1).reshape(-1), shards)
    cen_send, neg_got, hot_in, hot_out = lax.optimization_barrier((cen_send, neg_got, hot_in, hot_out))
    cen_got = exchange(cen_send, shards)
    con_send = gather_rows(out_shard, jnp.minimum(con_local, shard_rows - 1).reshape(-1), shards)
    con_send, cen_got = after(con_send, cen_got)
    con_got = exchange(con_send, shards)

    taken_by_con = lax.sort(taken - me * shard_rows * pack)
    taken_by_cen = lax.sort((taken % pack) * (2 * shard_rows) + taken // pack - me * shard_rows)
    num_taken = jnp.sum((taken % pack < hot).astype(jnp.int32))
    base_out, = pair_sums([hot_in], [out_shard], jnp.minimum(taken_by_con % pack, hot - 1), taken_by_con // pack, num_taken, True)
    ship_hot, = pair_sums([out_shard], [hot_in], jnp.minimum(taken_by_cen % (2 * shard_rows), shard_rows - 1), taken_by_cen // (2 * shard_rows), num_taken)

    neg_times = jnp.concatenate([hot_times(negative_ids, hot), neg_times])
    hot_cen_times = hot_times(center_ids, hot)
    w_half, w_high, w_low = split_rows([hot_out, neg_got], neg_times)
    uh_half, uh_high, uh_low = split_rows([hot_in], hot_cen_times)
    uc_half, uc_high, uc_low = split_rows([cen_got], cen_times)

    def neg_grads(u_half):
        return (NEG_WEIGHT / num_negs * jax.nn.sigmoid(dot(u_half, w_half, ((1,), (1,))))).astype(jnp.bfloat16)

    grad_h, grad_c = neg_grads(uh_half), neg_grads(uc_half)
    rows_in, cols_in = ((0,), (0,)), ((1,), (0,))

    def rest(times, half, high, low):
        return (times.astype(jnp.float32)[:, None] * half.astype(jnp.float32) - high.astype(jnp.float32) - low.astype(jnp.float32)).astype(jnp.bfloat16)

    d_neg = dot(grad_h, uh_high, rows_in) + dot(grad_h, uh_low, rows_in) + dot(grad_c, uc_high, rows_in)
    more = (jnp.max(cen_times) > 2) | (jnp.max(hot_cen_times) > 256)
    d_neg = when(more, lambda d: d + dot(grad_c, uc_low, rows_in) + dot(grad_h, rest(hot_cen_times, uh_half, uh_high, uh_low), rows_in) + dot(grad_c, rest(cen_times, uc_half, uc_high, uc_low), rows_in), d_neg)
    d_neg = jnp.where(neg_times[:, None] > 0, neg_times.astype(jnp.float32)[:, None] * d_neg, 0.0)
    neg_part, neg_hot = d_neg[hot:], d_neg[:hot]

    con_hot, con_part = pair_sums([hot_in, cen_got], [hot_out, con_got], cen_by_con, con_cell, num_stay)
    cen_hot, cen_part = pair_sums([hot_out, con_got], [hot_in, cen_got], con_by_cen, cen_order, num_stay)

    def center_grads(grad, times, pair_part):
        d = dot(grad, w_high, cols_in) + dot(grad[:, :hot], w_low[:hot], cols_in)
        more = (jnp.max(neg_times[hot:]) > 2) | (jnp.max(neg_times) > 256)
        d = when(more, lambda d: d + dot(grad[:, hot:], w_low[hot:], cols_in) + dot(grad, rest(neg_times, w_half, w_high, w_low), cols_in), d)
        return jnp.where(times[:, None] > 0, times.astype(jnp.float32)[:, None] * d + pair_part, 0.0)

    cen_hot = center_grads(grad_h, hot_cen_times, cen_hot) + ship_hot
    cen_part = center_grads(grad_c, cen_times, cen_part)

    neg_part, con_got = after(neg_part, con_got)
    neg_back = exchange(neg_part, shards)
    con_part, neg_back = after(con_part, neg_back)
    con_back = exchange(con_part, shards)
    out_hot = lax.psum(con_hot + neg_hot, AXIS_NAME)
    cen_part, con_back, out_hot, cen_hot = lax.optimization_barrier((cen_part, con_back, out_hot, cen_hot))
    cen_back = exchange(cen_part, shards)
    out_hot = jnp.where(me == 0, out_hot, 0.0)
    in_hot = lax.psum(cen_hot, AXIS_NAME)
    in_hot = jnp.where(me == 0, in_hot, 0.0)
    new_out = subtract_rows(base_out, out_hot, [(neg_local, neg_back), (con_local, con_back)])
    new_in = subtract_rows(in_shard, in_hot, [(cen_local, cen_back)])
    return new_in, new_out, all_fit


def solution(mesh):
    shards = mesh.shape[AXIS_NAME]

    def device_step(*args):
        new_in, new_out, all_fit = tight_step(shards, *args)
        return when(~all_fit, lambda _: full_step(shards, *args), (new_in, new_out))

    return jax.shard_map(device_step, mesh=mesh, in_specs=(P(AXIS_NAME, None), P(AXIS_NAME, None), P(AXIS_NAME), P(AXIS_NAME), P(AXIS_NAME)), out_specs=(P(AXIS_NAME, None), P(AXIS_NAME, None)), check_vma=False)
```

```python
import functools

import jax
import jax.numpy as jnp
from jax import lax
from jax.experimental import pallas as pl
from jax.experimental.pallas import tpu as pltpu
from jax.sharding import PartitionSpec as P


LEARN_RATE = 1.0
NEG_WEIGHT = 5.0
AXIS_NAME = 'vp'
HOT_ROWS = 768
LANES = 128
SUBLANES = 8
PAIR_TILES = 4
NO_ID = 2**30
VMEM_BYTES = 60 * 2**20
ANY = pl.BlockSpec(memory_space=pl.ANY)


def unique_capacity(num_ids, shards):
    common_slots = 3 * num_ids // shards
    return common_slots // 4 + (num_ids - common_slots + shards - 1) // shards


def context_capacity(num_ids, shards):
    share = tight_capacity(num_ids, shards) * 5 // 8
    return share + 56, tight_capacity(num_ids, shards) - share + 64


def tight_capacity(num_ids, shards):
    return (num_ids - 3 * num_ids // shards + shards - 1) // shards


def tile_view(rows):
    n, d = rows.shape
    return rows.reshape(n // SUBLANES, SUBLANES, d // LANES, LANES).transpose(0, 2, 1, 3).reshape(n * d // LANES, LANES)


def row_view(lines, d):
    n = lines.shape[0] * LANES // d
    return lines.reshape(n // SUBLANES, d // LANES, SUBLANES, LANES).transpose(0, 2, 1, 3).reshape(n, d)


def first_line(row, d):
    return (row // SUBLANES) * (SUBLANES * (d // LANES)) + row % SUBLANES


def gather_rows(table, rows, groups):
    n, d = rows.shape[0], table.shape[1]
    chunks, cap = d // LANES, n // groups
    view = tile_view(table)

    def body(line, t_ref, o_ref):
        group = pl.program_id(0)

        def step(t, carry):
            start = group * cap + t * SUBLANES
            got = [t_ref[pl.ds(line[start + j], chunks, stride=SUBLANES), :] for j in range(SUBLANES)]
            for j in range(SUBLANES):
                o_ref[pl.ds(t * SUBLANES * chunks + j, chunks, stride=SUBLANES), :] = got[j]
            return carry

        lax.fori_loop(0, cap // SUBLANES, step, 0, unroll=2 if cap % (2 * SUBLANES) == 0 else 1)

    out = pl.pallas_call(
        body,
        grid_spec=pltpu.PrefetchScalarGridSpec(
            num_scalar_prefetch=1, grid=(groups,),
            in_specs=[pl.BlockSpec(view.shape, lambda s, i: (0, 0), pipeline_mode=pl.Buffered(1))],
            out_specs=pl.BlockSpec((cap * chunks, LANES), lambda s, i: (s, 0))),
        out_shape=jax.ShapeDtypeStruct((n * chunks, LANES), table.dtype),
        cost_estimate=pl.CostEstimate(flops=0, bytes_accessed=4 * d * (table.shape[0] + 3 * n), transcendentals=0),
        compiler_params=pltpu.CompilerParams(vmem_limit_bytes=VMEM_BYTES),
        name='gather_rows',
    )(first_line(rows, d), view)
    return row_view(out, d)


def pair_sums(x_parts, y_parts, x_row, y_row, count, from_y=False):
    d = x_parts[0].shape[1]
    chunks, per_step = d // LANES, PAIR_TILES * SUBLANES
    views = [tile_view(a) for a in x_parts + y_parts]
    num_x, num_y = len(x_parts), len(y_parts)
    sizes = [v.shape[0] for v in views]
    x_lines, y_lines = sum(sizes[:num_x]), sum(sizes[num_x:])
    y_size = y_lines + SUBLANES * chunks
    y_starts = [sum(sizes[num_x:num_x + k]) for k in range(num_y)]

    def body(*refs):
        number, x_line, y_line = refs[:3]
        ins = refs[3:3 + num_x + num_y]
        outs = refs[3 + num_x + num_y:3 + num_x + 2 * num_y]
        x_all, y_all, total, prod, sem = refs[3 + num_x + 2 * num_y:]
        copies = []
        for k, ref in enumerate(ins):
            start = sum(sizes[:k]) if k < num_x else y_starts[k - num_x]
            held = x_all if k < num_x else y_all
            copies.append(pltpu.make_async_copy(ref, held.at[pl.ds(start, sizes[k])], sem.at[k]))
            if from_y and k >= num_x:
                copies.append(pltpu.make_async_copy(ref, total.at[pl.ds(start, sizes[k])], sem.at[k + num_y]))
        for copy in copies:
            copy.start()

        def zero(t, carry):
            total[pl.ds(pl.multiple_of(t * 64, 64), 64), :] = jnp.zeros((64, LANES), jnp.float32)
            return carry

        if not from_y:
            lax.fori_loop(0, y_lines // 64, zero, 0)
        for copy in copies:
            copy.wait()

        def step(t, carry):
            run, last = carry
            kept, lines, grads = [], [], []
            for i in range(per_step):
                tile, j = i // SUBLANES, i % SUBLANES
                line = y_line[t * per_step + i]
                x = x_all[pl.ds(x_line[t * per_step + i], chunks, stride=SUBLANES), :]
                y = y_all[pl.ds(line, chunks, stride=SUBLANES), :]
                prod[pl.ds(tile * SUBLANES * chunks + j, chunks, stride=SUBLANES), :] = x * y
                kept.append(x)
                lines.append(line)
            for tile in range(PAIR_TILES):
                part = prod[pl.ds(tile * SUBLANES * chunks, SUBLANES), :]
                for k in range(1, chunks):
                    part = part + prod[pl.ds((tile * chunks + k) * SUBLANES, SUBLANES), :]
                score = jnp.broadcast_to(jnp.sum(part, axis=1, keepdims=True), (SUBLANES, LANES))
                grads.append(jax.nn.sigmoid(score) - 1.0)
            for i in range(per_step):
                tile, j = i // SUBLANES, i % SUBLANES
                same = (lines[i] == last).astype(jnp.float32)
                run = run * same + jnp.broadcast_to(grads[tile][j:j + 1, :], (chunks, LANES)) * kept[i]
                at = pl.ds(lines[i], chunks, stride=SUBLANES)
                total[at, :] = y_all[at, :] - LEARN_RATE * run if from_y else run
                last = lines[i]
            return run, last

        lax.fori_loop(0, pl.cdiv(number[0], per_step), step, (jnp.zeros((chunks, LANES), jnp.float32), jnp.int32(-1)))
        copies = [pltpu.make_async_copy(total.at[pl.ds(y_starts[k], sizes[num_x + k])], outs[k], sem.at[k]) for k in range(num_y)]
        for copy in copies:
            copy.start()
        for copy in copies:
            copy.wait()

    results = pl.pallas_call(
        body,
        grid_spec=pltpu.PrefetchScalarGridSpec(
            num_scalar_prefetch=3, grid=(1,), in_specs=[ANY] * (num_x + num_y), out_specs=[ANY] * num_y,
            scratch_shapes=[pltpu.VMEM((x_lines, LANES), jnp.float32), pltpu.VMEM((y_size, LANES), jnp.float32),
                            pltpu.VMEM((y_size, LANES), jnp.float32), pltpu.VMEM((per_step * chunks, LANES), jnp.float32),
                            pltpu.SemaphoreType.DMA((num_x + 2 * num_y,))]),
        out_shape=[jax.ShapeDtypeStruct((n, LANES), jnp.float32) for n in sizes[num_x:]],
        cost_estimate=pl.CostEstimate(flops=0, bytes_accessed=8 * 4 * d * x_row.shape[0], transcendentals=0),
        compiler_params=pltpu.CompilerParams(vmem_limit_bytes=VMEM_BYTES),
        name='pair_sums',
    )(count.astype(jnp.int32).reshape(1), first_line(x_row, d), first_line(y_row, d), *views)
    return [row_view(r, d) for r in results]


def subtract_rows(table, hot, parts):
    d = table.shape[1]
    chunks = d // LANES
    groups = parts[0][0].shape[0]
    caps = [rows.shape[1] for rows, _ in parts]
    view, hot_view = tile_view(table), tile_view(hot)
    lines = view.shape[0]
    count = len(parts)

    def body(*refs):
        line = refs[:count]
        t_hbm, h_ref = refs[count:count + 2]
        values = refs[count + 2:2 * count + 2]
        o_hbm, held, sem = refs[2 * count + 2:]
        group = pl.program_id(0)

        @pl.when(group == 0)
        def _():
            copy = pltpu.make_async_copy(t_hbm, held.at[pl.ds(0, lines)], sem)
            copy.start()
            copy.wait()

            def hot_step(t, carry):
                window = pl.ds(pl.multiple_of(t * 64, 64), 64)
                held[window, :] = held[window, :] - LEARN_RATE * h_ref[window, :]
                return carry

            lax.fori_loop(0, h_ref.shape[0] // 64, hot_step, 0)

        for p in range(count):
            batch = 16 if caps[p] % 16 == 0 else SUBLANES

            def step(t, carry, p=p, batch=batch):
                at = [line[p][group * caps[p] + t * batch + j] for j in range(batch)]
                new = []
                for j in range(batch):
                    source = (t * (batch // SUBLANES) + j // SUBLANES) * SUBLANES * chunks + j % SUBLANES
                    value = values[p][pl.ds(source, chunks, stride=SUBLANES), :]
                    new.append(held[pl.ds(at[j], chunks, stride=SUBLANES), :] - LEARN_RATE * value)
                for j in range(batch):
                    held[pl.ds(at[j], chunks, stride=SUBLANES), :] = new[j]
                return carry

            lax.fori_loop(0, caps[p] // batch, step, 0)

        @pl.when(group == groups - 1)
        def _():
            copy = pltpu.make_async_copy(held.at[pl.ds(0, lines)], o_hbm, sem)
            copy.start()
            copy.wait()

    out = pl.pallas_call(
        body,
        grid_spec=pltpu.PrefetchScalarGridSpec(
            num_scalar_prefetch=count, grid=(groups,),
            in_specs=[ANY, pl.BlockSpec(hot_view.shape, lambda s, *i: (0, 0))] + [pl.BlockSpec((c * chunks, LANES), lambda s, *i: (s, 0)) for c in caps],
            out_specs=ANY,
            scratch_shapes=[pltpu.VMEM((lines + SUBLANES * chunks, LANES), jnp.float32), pltpu.SemaphoreType.DMA]),
        out_shape=jax.ShapeDtypeStruct((lines, LANES), jnp.float32),
        cost_estimate=pl.CostEstimate(flops=0, bytes_accessed=4 * d * (2 * table.shape[0] + 3 * groups * sum(caps)), transcendentals=0),
        compiler_params=pltpu.CompilerParams(vmem_limit_bytes=VMEM_BYTES),
        name='subtract_rows',
    )(*[first_line(rows.reshape(-1), d) for rows, _ in parts], view, hot_view, *[tile_view(values) for _, values in parts])
    return row_view(out, d)


def split_rows(sources, times, block=256):
    d = sources[0].shape[1]
    blocks = [a.shape[0] // block for a in sources]
    starts = [sum(blocks[:k]) for k in range(len(blocks))]
    total = sum(blocks) * block

    def body(*refs):
        ins, t_ref, (r_ref, h_ref, l_ref) = refs[:len(sources)], refs[len(sources)], refs[len(sources) + 1:]
        step = pl.program_id(0)
        for k, ref in enumerate(ins):
            @pl.when((step >= starts[k]) & (step < starts[k] + blocks[k]))
            def _(ref=ref):
                rounded = ref[...].astype(jnp.bfloat16)
                scaled = rounded.astype(jnp.float32) * t_ref[...]
                high = scaled.astype(jnp.bfloat16)
                r_ref[...] = rounded
                h_ref[...] = high
                l_ref[...] = (scaled - high.astype(jnp.float32)).astype(jnp.bfloat16)

    def pick(k):
        return lambda i: (jnp.clip(i - starts[k], 0, blocks[k] - 1), 0)

    spec = pl.BlockSpec((block, d), lambda i: (i, 0))
    return pl.pallas_call(
        body, grid=(sum(blocks),),
        in_specs=[pl.BlockSpec((block, d), pick(k)) for k in range(len(sources))] + [pl.BlockSpec((block, 1), lambda i: (i, 0))],
        out_specs=[spec] * 3, out_shape=[jax.ShapeDtypeStruct((total, d), jnp.bfloat16)] * 3,
        cost_estimate=pl.CostEstimate(flops=0, bytes_accessed=10 * d * total, transcendentals=0),
        name='split_rows',
    )(*sources, times.astype(jnp.float32)[:, None])


def running_count(flags):
    rows = flags.shape[0] // LANES
    grid = flags.reshape(rows, LANES).astype(jnp.bfloat16)
    upper = (jnp.arange(LANES)[:, None] <= jnp.arange(LANES)[None, :]).astype(jnp.bfloat16)
    inner = jnp.dot(grid, upper, preferred_element_type=jnp.float32)
    lower = (jnp.arange(rows)[:, None] > jnp.arange(rows)[None, :]).astype(jnp.bfloat16)
    outer = jnp.dot(lower, inner[:, -1:].astype(jnp.bfloat16), preferred_element_type=jnp.float32)
    return (inner + outer).astype(jnp.int32).reshape(-1)


def mark_unique(sorted_ids, shard_rows, shards, hot, limit=NO_ID):
    previous = jnp.concatenate([jnp.full((1,), -1, jnp.int32), sorted_ids[:-1]])
    first = (sorted_ids != previous) & (sorted_ids >= hot) & (sorted_ids < limit)
    owner = sorted_ids // shard_rows
    rank = running_count(first) - 1
    owners = jnp.arange(shards, dtype=jnp.int32)
    counts = jnp.sum((first[None, :] & (owner[None, :] == owners[:, None])).astype(jnp.int32), axis=1)
    starts = jnp.sum(jnp.where(owners[None, :] < owners[:, None], counts[None, :], 0), axis=1)
    start_of = jnp.sum(jnp.where(owner[None, :] == owners[:, None], starts[:, None], 0), axis=0)
    return first, owner, rank - start_of, counts


def fill_cells(counts, capacity, shards):
    owners = jnp.arange(shards, dtype=jnp.int32)[:, None]
    slot = jnp.arange(capacity, dtype=jnp.int32)[None, :]
    return jnp.where(slot >= counts[:, None], owners * capacity + slot, NO_ID).reshape(-1)


def spread(values, capacity):
    return jnp.broadcast_to(values[:, None], (values.shape[0], capacity)).reshape(-1)


def ask_lists(sorted_ids, first, owner, rank, counts, shard_rows, shards, capacity):
    num_ids = sorted_ids.shape[0]
    cells = shards * capacity
    pack = 2 * num_ids
    key = jnp.where(first & (rank < capacity), owner * capacity + rank, NO_ID)
    past = (jnp.arange(shards, dtype=jnp.int32) + 1) * shard_rows
    ends = jnp.sum((sorted_ids[None, :] < past[:, None]).astype(jnp.int32), axis=1)
    packed = lax.sort((
        jnp.concatenate([key, fill_cells(counts, capacity, shards)]),
        jnp.concatenate([sorted_ids * pack + jnp.arange(num_ids, dtype=jnp.int32), spread(past * pack + ends, capacity)])), num_keys=1)[1][:cells]
    places = packed % pack
    times = jnp.concatenate([places[1:], jnp.full((1,), num_ids, jnp.int32)]) - places
    return (packed // pack).reshape(shards, capacity), times


def hot_times(ids, hot):
    return jnp.sum((ids[None, :] == jnp.arange(hot, dtype=jnp.int32)[:, None]).astype(jnp.int32), axis=1)


def cell_of(sorted_ids, owner, rank, shards, hot, capacity):
    return jnp.where(sorted_ids < hot, sorted_ids, jnp.minimum(hot + owner * capacity + rank, hot + shards * capacity - 1))


def exchange(rows, shards):
    return lax.all_to_all(rows.reshape(shards, -1, rows.shape[-1]), AXIS_NAME, 0, 0).reshape(rows.shape)


def exchange_ids(ids):
    return lax.all_to_all(ids, AXIS_NAME, 0, 0)


def dot(a, b, dims):
    return lax.dot_general(a, b, (dims, ((), ())), preferred_element_type=jnp.float32)


def after(value, earlier):
    return lax.optimization_barrier((value, earlier))


def when(predicate, update, value):
    return lax.while_loop(lambda state: state[0], lambda state: (jnp.zeros((), jnp.bool_), update(state[1])), (predicate, value))[1]


def plan_unique(sorted_ids, shard_rows, shards, capacity):
    previous = jnp.concatenate([jnp.full((1,), -1, jnp.int32), sorted_ids[:-1]])
    first = (sorted_ids != previous)
    owner = sorted_ids // shard_rows
    rank = running_count(first) - 1
    owners = jnp.arange(shards, dtype=jnp.int32)
    counts = jnp.sum((first[None, :] & (owner[None, :] == owners[:, None])).astype(jnp.int32), axis=1)
    starts = jnp.sum(jnp.where(owners[None, :] < owners[:, None], counts[None, :], 0), axis=1)
    start_of = jnp.sum(jnp.where(owner[:, None] == owners[None, :], starts[None, :], 0), axis=1)
    packed = lax.sort(jnp.where(first, sorted_ids, jnp.int32(NO_ID)))
    packed = jnp.concatenate([packed, jnp.full((capacity,), NO_ID, jnp.int32)])
    asked = jnp.stack([lax.dynamic_slice(packed, (starts[s],), (capacity,)) for s in range(shards)])
    return owner, rank - start_of, asked


def full_step(shards, in_shard, out_shard, center_ids, context_ids, negative_ids):
    shard_rows = in_shard.shape[0]
    num_pairs, num_negs = center_ids.shape[0], negative_ids.shape[0]
    cap_pairs, cap_negs = unique_capacity(num_pairs, shards), unique_capacity(num_negs, shards)
    me = lax.axis_index(AXIS_NAME)
    take = functools.partial(jnp.take, axis=0, mode='clip')
    neg_sorted = lax.sort(negative_ids)
    cen_sorted, con_moved = lax.sort((center_ids, context_ids), num_keys=1)
    con_sorted, con_pos = lax.sort((con_moved, jnp.arange(num_pairs, dtype=jnp.int32)), num_keys=1)

    def fetch(table, sorted_ids, capacity):
        owner, rank, asked = plan_unique(sorted_ids, shard_rows, shards, capacity)
        local = jnp.clip(exchange_ids(asked) - me * shard_rows, 0, shard_rows - 1).reshape(-1)
        return owner * capacity + rank, local, exchange(take(table, local), shards)

    neg_cell, neg_local, neg_got = fetch(out_shard, neg_sorted, cap_negs)
    cen_cell, cen_local, cen_got = fetch(in_shard, cen_sorted, cap_pairs)
    con_cell, con_local, con_got = fetch(out_shard, con_sorted, cap_pairs)
    con_cell = lax.sort((con_pos, con_cell), num_keys=1)[1]
    negative_half = split_rows([take(neg_got, neg_cell)], jnp.ones((num_negs,), jnp.float32))[0]
    center_vec = take(cen_got, cen_cell)
    center_half = split_rows([center_vec], jnp.ones((num_pairs,), jnp.float32))[0]
    neg_grad = (NEG_WEIGHT / num_negs * jax.nn.sigmoid(dot(center_half, negative_half, ((1,), (1,))))).astype(jnp.bfloat16)
    context_vec = take(con_got, con_cell)
    pos_grad = (jax.nn.sigmoid(jnp.sum(center_vec * context_vec, axis=1)) - 1.0)[:, None]
    d_center = dot(neg_grad, negative_half, ((1,), (0,))) + pos_grad * context_vec
    d_negative = dot(neg_grad, center_half, ((0,), (0,)))

    def give(table, grads, cell, local, capacity):
        sums = jax.ops.segment_sum(grads, cell, num_segments=shards * capacity)
        return table.at[local].add(-LEARN_RATE * exchange(sums, shards))

    new_out = give(out_shard, d_negative, neg_cell, neg_local, cap_negs)
    new_out = give(new_out, pos_grad * center_vec, con_cell, con_local, cap_pairs)
    return give(in_shard, d_center, cen_cell, cen_local, cap_pairs), new_out


def tight_step(shards, in_shard, out_shard, center_ids, context_ids, negative_ids):
    shard_rows = in_shard.shape[0]
    num_pairs, num_negs = center_ids.shape[0], negative_ids.shape[0]
    hot = HOT_ROWS
    cap_pairs, cap_negs = tight_capacity(num_pairs, shards), tight_capacity(num_negs, shards)
    me = lax.axis_index(AXIS_NAME)

    hot_both = jnp.concatenate([in_shard[:hot], out_shard[:hot]])
    hot_both = lax.psum(jnp.where(me == 0, hot_both, 0.0), AXIS_NAME)
    hot_in, hot_out = hot_both[:hot], hot_both[hot:]

    neg_sorted = lax.sort(negative_ids)
    neg_first, neg_owner, neg_rank, neg_counts = mark_unique(neg_sorted, shard_rows, shards, hot)
    neg_asked, neg_times = ask_lists(neg_sorted, neg_first, neg_owner, neg_rank, neg_counts, shard_rows, shards, cap_negs)

    cen_sorted, con_moved = lax.sort((center_ids, context_ids), num_keys=1)
    cen_first, cen_owner, cen_rank, cen_counts = mark_unique(cen_sorted, shard_rows, shards, hot)
    cen_asked, cen_times = ask_lists(cen_sorted, cen_first, cen_owner, cen_rank, cen_counts, shard_rows, shards, cap_pairs)
    cen_cell = cell_of(cen_sorted, cen_owner, cen_rank, shards, hot, cap_pairs)
    cap_con, cap_ship = context_capacity(num_pairs, shards)
    past_all = shards * shard_rows
    sent = (cen_sorted < hot) & (con_moved >= hot)
    con_keys, cen_by_con = lax.sort((con_moved + jnp.where(sent, past_all, 0), cen_cell), num_keys=1)
    stays = con_keys < past_all
    num_stay = jnp.sum(stays.astype(jnp.int32))
    con_first, con_owner, con_rank, con_counts = mark_unique(con_keys, shard_rows, shards, hot, past_all)
    con_cell = jnp.where(stays, cell_of(con_keys, con_owner, con_rank, shards, hot, cap_con), hot + shards * cap_con)
    sent_center = cen_by_con
    cen_key = jnp.where(stays, cen_by_con, hot + shards * cap_pairs)
    cen_by_con = jnp.where(stays, cen_by_con, 0)
    owners = jnp.arange(shards, dtype=jnp.int32)
    past = (owners + 1) * shard_rows
    ship_owner = con_owner - shards
    ship_upto = jnp.sum((con_keys[None, :] < (past + past_all)[:, None]).astype(jnp.int32), axis=1)
    ship_from = jnp.sum((con_keys[None, :] < (past - shard_rows + past_all)[:, None]).astype(jnp.int32), axis=1)
    ship_counts = ship_upto - ship_from
    from_of = jnp.sum(jnp.where(ship_owner[None, :] == owners[:, None], ship_from[:, None], 0), axis=0)
    ship_rank = jnp.arange(num_pairs, dtype=jnp.int32) - from_of
    con_cells = shards * cap_con
    key = jnp.where(con_first & (con_rank < cap_con), con_owner * cap_con + con_rank, NO_ID)
    key = jnp.where(stays | (ship_rank >= cap_ship), key, con_cells + ship_owner * cap_ship + ship_rank)
    ship_fill = fill_cells(ship_counts, cap_ship, shards)
    pack = 2 * hot
    both = lax.sort((
        jnp.concatenate([key, fill_cells(con_counts, cap_con, shards), jnp.where(ship_fill < NO_ID, con_cells + ship_fill, NO_ID)]),
        jnp.concatenate([jnp.where(stays, con_keys, (con_keys - past_all) * pack + sent_center), spread(past, cap_con), spread(past * pack + hot, cap_ship)])), num_keys=1)[1]
    con_asked = both[:con_cells].reshape(shards, cap_con)
    shipped = both[con_cells:con_cells + shards * cap_ship].reshape(shards, cap_ship)
    over = (neg_counts > cap_negs) | (cen_counts > cap_pairs) | (con_counts > cap_con) | (ship_counts > cap_ship)
    spill = jnp.broadcast_to(over.astype(jnp.int32)[None, :], (shards, shards))
    asked = exchange_ids(jnp.concatenate([cen_asked, con_asked, neg_asked, shipped, spill], axis=1))
    all_fit = jnp.sum(asked[:, -shards:]) == 0
    cuts = [0, cap_pairs, cap_pairs + cap_con, cap_pairs + cap_con + cap_negs, asked.shape[1] - shards]
    cen_local, con_local, neg_local = [asked[:, cuts[k]:cuts[k + 1]] - me * shard_rows for k in range(3)]
    taken = asked[:, cuts[3]:cuts[4]].reshape(-1)
    neg_send = gather_rows(out_shard, jnp.minimum(neg_local, shard_rows - 1).reshape(-1), shards)
    neg_got = exchange(neg_send, shards)
    cen_order, con_by_cen = lax.sort((cen_key, jnp.where(stays, con_cell, 0)), num_keys=1)

    cen_send = gather_rows(in_shard, jnp.minimum(cen_local, shard_rows - 1).reshape(-1), shards)
    cen_send, neg_got, hot_in, hot_out = lax.optimization_barrier((cen_send, neg_got, hot_in, hot_out))
    cen_got = exchange(cen_send, shards)
    con_send = gather_rows(out_shard, jnp.minimum(con_local, shard_rows - 1).reshape(-1), shards)
    con_send, cen_got = after(con_send, cen_got)
    con_got = exchange(con_send, shards)

    taken_by_con = lax.sort(taken - me * shard_rows * pack)
    taken_by_cen = lax.sort((taken % pack) * (2 * shard_rows) + taken // pack - me * shard_rows)
    num_taken = jnp.sum((taken % pack < hot).astype(jnp.int32))
    base_out, = pair_sums([hot_in], [out_shard], jnp.minimum(taken_by_con % pack, hot - 1), taken_by_con // pack, num_taken, True)
    ship_hot, = pair_sums([out_shard], [hot_in], jnp.minimum(taken_by_cen % (2 * shard_rows), shard_rows - 1), taken_by_cen // (2 * shard_rows), num_taken)

    neg_times = jnp.concatenate([hot_times(negative_ids, hot), neg_times])
    hot_cen_times = hot_times(center_ids, hot)
    w_half, w_high, w_low = split_rows([hot_out, neg_got], neg_times)
    uh_half, uh_high, uh_low = split_rows([hot_in], hot_cen_times)
    uc_half, uc_high, uc_low = split_rows([cen_got], cen_times)

    def neg_grads(u_half):
        return (NEG_WEIGHT / num_negs * jax.nn.sigmoid(dot(u_half, w_half, ((1,), (1,))))).astype(jnp.bfloat16)

    grad_h, grad_c = neg_grads(uh_half), neg_grads(uc_half)
    rows_in, cols_in = ((0,), (0,)), ((1,), (0,))

    def rest(times, half, high, low):
        return (times.astype(jnp.float32)[:, None] * half.astype(jnp.float32) - high.astype(jnp.float32) - low.astype(jnp.float32)).astype(jnp.bfloat16)

    d_neg = dot(grad_h, uh_high, rows_in) + dot(grad_h, uh_low, rows_in) + dot(grad_c, uc_high, rows_in)
    more = (jnp.max(cen_times) > 2) | (jnp.max(hot_cen_times) > 256)
    d_neg = when(more, lambda d: d + dot(grad_c, uc_low, rows_in) + dot(grad_h, rest(hot_cen_times, uh_half, uh_high, uh_low), rows_in) + dot(grad_c, rest(cen_times, uc_half, uc_high, uc_low), rows_in), d_neg)
    d_neg = jnp.where(neg_times[:, None] > 0, neg_times.astype(jnp.float32)[:, None] * d_neg, 0.0)
    neg_part, neg_hot = d_neg[hot:], d_neg[:hot]

    con_hot, con_part = pair_sums([hot_in, cen_got], [hot_out, con_got], cen_by_con, con_cell, num_stay)
    cen_hot, cen_part = pair_sums([hot_out, con_got], [hot_in, cen_got], con_by_cen, cen_order, num_stay)

    def center_grads(grad, times, pair_part):
        d = dot(grad, w_high, cols_in) + dot(grad[:, :hot], w_low[:hot], cols_in)
        more = (jnp.max(neg_times[hot:]) > 2) | (jnp.max(neg_times) > 256)
        d = when(more, lambda d: d + dot(grad[:, hot:], w_low[hot:], cols_in) + dot(grad, rest(neg_times, w_half, w_high, w_low), cols_in), d)
        return jnp.where(times[:, None] > 0, times.astype(jnp.float32)[:, None] * d + pair_part, 0.0)

    cen_hot = center_grads(grad_h, hot_cen_times, cen_hot) + ship_hot
    cen_part = center_grads(grad_c, cen_times, cen_part)

    neg_part, con_got = after(neg_part, con_got)
    neg_back = exchange(neg_part, shards)
    con_part, neg_back = after(con_part, neg_back)
    con_back = exchange(con_part, shards)
    out_hot = lax.psum(con_hot + neg_hot, AXIS_NAME)
    cen_part, con_back, out_hot, cen_hot = lax.optimization_barrier((cen_part, con_back, out_hot, cen_hot))
    cen_back = exchange(cen_part, shards)
    out_hot = jnp.where(me == 0, out_hot, 0.0)
    in_hot = lax.psum(cen_hot, AXIS_NAME)
    in_hot = jnp.where(me == 0, in_hot, 0.0)
    new_out = subtract_rows(base_out, out_hot, [(neg_local, neg_back), (con_local, con_back)])
    new_in = subtract_rows(in_shard, in_hot, [(cen_local, cen_back)])
    return new_in, new_out, all_fit


def solution(mesh):
    shards = mesh.shape[AXIS_NAME]

    def device_step(*args):
        new_in, new_out, all_fit = tight_step(shards, *args)
        return when(~all_fit, lambda _: full_step(shards, *args), (new_in, new_out))

    return jax.shard_map(device_step, mesh=mesh, in_specs=(P(AXIS_NAME, None), P(AXIS_NAME, None), P(AXIS_NAME), P(AXIS_NAME), P(AXIS_NAME)), out_specs=(P(AXIS_NAME, None), P(AXIS_NAME, None)), check_vma=False)
```
